32 devices in a mesh: groups: 2 (over y), seq: 8 (over z, x), tp: 2 (over core).
Axes of the slice: x: 2, y: 2, z: 4, core: 2. Of those that a mesh axis runs over, the one named last changes fastest.
Arguments:
- span_queries: bfloat16 [128, 64, 128], P(('groups', 'seq'), 'tp'), parts along dimension 0, may hold values from -180 to 180
- span_keys: bfloat16 [128, 4, 128], P(('groups', 'seq'), 'tp'), parts along dimension 0, may hold values from -9 to 9
- span_values: bfloat16 [128, 4, 128], P(('groups', 'seq'), 'tp'), parts along dimension 0, may hold values from -6.5 to 6.5
- prefix_keys: bfloat16 [1152, 4, 128], P(('groups', 'seq'), 'tp'), parts along dimension 0, may hold values from -9 to 9
- prefix_values: bfloat16 [1152, 4, 128], P(('groups', 'seq'), 'tp'), parts along dimension 0, may hold values from -6.5 to 6.5
- prefix_lengths: int32 [16], P('groups'), parts along dimension 0, may hold values from 1 to 72
- decode_queries: bfloat16 [32, 64, 128], P(('groups', 'seq'), 'tp'), parts along dimension 0, may hold values from -180 to 180
- decode_new_keys: bfloat16 [32, 4, 128], P(('groups', 'seq'), 'tp'), parts along dimension 0, may hold values from -6 to 6
- decode_new_values: bfloat16 [32, 4, 128], P(('groups', 'seq'), 'tp'), parts along dimension 0, may hold values from -6 to 6
- decode_key_cache: bfloat16 [64, 256, 4, 128], P(('groups', 'seq'), None, 'tp'), parts along dimension 0, may hold values from -6 to 6
- decode_value_cache: bfloat16 [64, 256, 4, 128], P(('groups', 'seq'), None, 'tp'), parts along dimension 0, may hold values from -6 to 6
- owner_map: int32 [32, 1], P('groups'), parts along dimension 0, may hold values from 0 to 7; in each aligned block of 16 rows (0 to 15, 16 to 31, ...) at most 4 rows name the same one
- decode_lengths: int32 [32], P('groups'), parts along dimension 0, may hold values from 1 to 256
Outputs:
- prefill_out: bfloat16 [128, 64, 128], P(('groups', 'seq'), 'tp'), parts along dimension 0
- decode_out: bfloat16 [64, 64, 128], P(('groups', 'seq'), 'tp'), parts along dimension 0
The draws below stay inside these ranges and needn't reach their ends.
There are 2 independent parts, one for each index of `groups`. The reference program is written for one: setup_inputs(seed, part) draws one part's arguments, and reference() takes and returns one part's arrays. A program takes and returns all parts, laid end to end along the dimension named above; each array names one. Nothing has to cross between parts.
Inputs may be any that keep to these rules, and one draw needn't show every extreme that they name: `owner_map`: no shard owns more than 4 requests, and some shard owns exactly 4.
All inputs are finite; a program needn't handle non-finite values.
Results may differ from the reference program's by a relative error of at most 0.005.
Values may be sent and summed in bfloat16 or wider, within the bound.
No kernel may reach another device: no remote copies, remote signals or barrier semaphores. Data moves between devices by JAX's collectives and lax.ppermute only.
A program may use at most 64 MiB of HBM per device.

```python
import math
import jax
import jax.numpy as jnp
import numpy as np
from jax import lax

H = 64
KVH = 4
HD = 128
CH_DEV = 8
PRE_DEV = 72
CTX = 256
SLOTS = 4
SPAN = 64
PREFIX = 576
REQS = 16
OWN = 32
N_SEQ = 8


def noisy_queries(key, rows):
    base = jax.random.truncated_normal(key, -4.0, 4.0, (rows, H, HD), jnp.float32) * 1.7
    return base.astype(jnp.bfloat16)


def shard_scales(key, blocks, marker, lower, upper):
    scale_key = jax.random.fold_in(key, marker)
    return jnp.exp(jax.random.uniform(scale_key, (blocks, 1, KVH, 1), jnp.float32, jnp.log(lower), jnp.log(upper)))


def scale_range():
    lower, upper = (0.3, 1.7)
    return (lower, upper)


def scaled_keys(key, rows, width, marker):
    blocks = rows // width
    lower, upper = scale_range()
    scales = shard_scales(key, blocks, marker, lower, upper)
    entries = jax.random.truncated_normal(jax.random.fold_in(key, marker + 1), -4.0, 4.0, (blocks, width, KVH, HD), jnp.float32)
    factor = jnp.exp(jax.random.uniform(jax.random.fold_in(key, marker + 2), (blocks, width, KVH, 1), jnp.float32, jnp.log(0.8), jnp.log(1.25)))
    return (entries * scales * factor).reshape(rows, KVH, HD).astype(jnp.bfloat16)


def offset_values(key, rows, width, marker):
    blocks = rows // width
    entries = jax.random.truncated_normal(jax.random.fold_in(key, marker + 3), -4.0, 4.0, (blocks, width, KVH, HD), jnp.float32)
    return entries.reshape(rows, KVH, HD).astype(jnp.bfloat16)


def draw_span_queries(key, part):
    return noisy_queries(jax.random.fold_in(key, 11), SPAN)


def draw_decode_queries(key, part):
    return noisy_queries(jax.random.fold_in(key, 13), REQS)


def draw_prefix_keys(key, part):
    return scaled_keys(key, PREFIX, PRE_DEV, 201)


def draw_prefix_values(key, part):
    return offset_values(key, PREFIX, PRE_DEV, 201)


def draw_span_keys(key, part):
    return scaled_keys(key, SPAN, CH_DEV, 301)


def draw_span_values(key, part):
    return offset_values(key, SPAN, CH_DEV, 301)


def set_ends(drawn, rng, least, high):
    longest = drawn.shape.index(max(drawn.shape))
    spots = []
    for shift in (0, 1):
        where = [jax.random.randint(jax.random.fold_in(rng, axis), (), 0, length) for axis, length in enumerate(drawn.shape)]
        where[longest] = (where[longest] + shift) % drawn.shape[longest]
        spots.append(tuple(where))
    return drawn.at[spots[0]].set(least).at[spots[1]].set(high)


def steps_of(own_key, shape, pieces, low, top_value):
    def one(axis_at, parts):
        heights = jax.random.uniform(jax.random.fold_in(jax.random.fold_in(own_key, 6), axis_at), (parts,), jnp.float32, low / len(pieces), top_value / len(pieces))
        return jnp.repeat(jnp.exp(heights), shape[axis_at] // parts).reshape((-1,) + (1,) * (len(shape) - axis_at - 1))

    loudness = one(*pieces[0])
    for cut in pieces[1:]:
        loudness = loudness * one(*cut)
    return loudness


def assign_block(key, own, number, rows, amount, top, bound, skew):
    order = jax.random.permutation(key, amount)
    packed, usual = shares(amount, rows * top, bound, skew, True), shares(amount, rows * top, bound, skew, False)
    places = jnp.arange(amount)

    def named(sizes, rotation):
        used = int((sizes > 0).sum())
        fixed = max(1, used // 4)
        passed = fixed + (places - fixed + rotation * (used - fixed)) % max(1, amount - fixed)
        return jnp.zeros((amount,), jnp.int32).at[order[jnp.where(places < fixed, places, passed)]].set(jnp.asarray(sizes, jnp.int32))

    sizes = jnp.where(number % 4 == 0, named(packed, number // 4), named(usual, number - number // 4 - 1))
    mixed = jax.random.permutation(jax.random.fold_in(own, 3), amount)
    giver, sink = mixed[0:amount // 2 * 2:2], mixed[1:amount // 2 * 2:2]
    margin = jnp.minimum(sizes[giver] - 1, bound - sizes[sink]) // 2
    margin = jnp.where((giver == order[0]) | (sink == order[0]) | (sizes[sink] == 0), 0, jnp.maximum(margin, 0))
    passed = jax.random.randint(jax.random.fold_in(own, 4), (amount // 2,), 0, 1 << 20) % (margin + 1)
    sizes = sizes.at[giver].add(-passed).at[sink].add(passed)
    items = jnp.searchsorted(jnp.cumsum(sizes), jnp.arange(rows * top), side="right").astype(jnp.int32)
    grid = items.reshape(top, rows).T
    grid = grid[jax.random.permutation(jax.random.fold_in(own, 1), rows)]
    rotation = jax.random.randint(jax.random.fold_in(own, 2), (rows, 1), 0, top)
    return jnp.take_along_axis(grid, (jnp.arange(top)[None, :] + rotation) % top, axis=1)


def shares(count, total, limit, slope, full):
    portions = [(1 << 20) // math.isqrt(grade ** slope) + 1 for grade in range(1, count + 1)]
    largest = limit if full else min(limit, max(-(-total // count), total * portions[0] // sum(portions)))
    least = 1 if total - largest >= count - 1 else 0
    holding, surplus = [largest] + [least] * (count - 1), total - largest - least * (count - 1)
    while surplus > 0:
        free = [i for i in range(1, count) if holding[i] < largest] or [i for i in range(1, count) if holding[i] < limit]
        pool, remaining = sum([portions[i] for i in free]), surplus
        for i in free:
            addition = min(limit - holding[i], max(1, remaining * portions[i] // pool), surplus)
            holding[i] = holding[i] + addition
            surplus = surplus - addition
    return np.array(holding)


def normal_values(key, shape, deviation, bound, cuts=(), kind=jnp.bfloat16):
    array = deviation * jax.random.normal(key, shape, jnp.float32)
    if cuts:
        array = array * steps_of(key, shape, cuts, -0.22, 0.18)
    return jnp.clip(array, -bound, bound).astype(kind)


def setup_inputs(seed: int = 0, part: int = 0) -> dict:
    key_of = jax.random.split(jax.random.key(seed), 14)
    part_splits = jax.random.split(jax.random.fold_in(key_of[13], part), 14)
    span_queries = draw_span_queries(jax.random.fold_in(jax.random.fold_in(key_of[13], part), 71), part)
    span_keys = draw_span_keys(jax.random.fold_in(jax.random.fold_in(key_of[13], part), 71), part)
    span_values = draw_span_values(jax.random.fold_in(jax.random.fold_in(key_of[13], part), 71), part)
    prefix_keys = draw_prefix_keys(jax.random.fold_in(jax.random.fold_in(key_of[13], part), 71), part)
    prefix_values = draw_prefix_values(jax.random.fold_in(jax.random.fold_in(key_of[13], part), 71), part)
    prefix_lengths = set_ends(jax.random.randint(part_splits[5], (N_SEQ,), 1, PRE_DEV + 1), jax.random.fold_in(part_splits[5], 1), 1, PRE_DEV).astype(jnp.int32)
    decode_queries = draw_decode_queries(jax.random.fold_in(jax.random.fold_in(key_of[13], part), 71), part)
    decode_new_keys = normal_values(part_splits[7], (REQS, KVH, HD), 1.7, 6.0, ((0, 8), (1, 2)))
    decode_new_values = normal_values(part_splits[8], (REQS, KVH, HD), 1.0, 6.0, ((0, 8), (1, 2)))
    decode_key_cache = normal_values(part_splits[9], (OWN, CTX, KVH, HD), 1.7, 6.0, ((0, 8), (2, 2)))
    decode_value_cache = normal_values(part_splits[10], (OWN, CTX, KVH, HD), 1.0, 6.0, ((0, 8), (2, 2)))
    owner_map_keys = jax.random.split(jax.random.fold_in(part_splits[11], 1), REQS // REQS)
    owner_map_turns = jax.random.permutation(jax.random.fold_in(part_splits[11], 3), REQS // REQS)
    owner_map = jax.vmap(lambda own, number: assign_block(jax.random.fold_in(part_splits[11], 2), own, number, REQS, N_SEQ, 1, SLOTS, 2))(owner_map_keys, owner_map_turns).reshape((REQS, 1))
    decode_lengths = set_ends(jax.random.randint(part_splits[12], (REQS,), 1, CTX + 1), jax.random.fold_in(part_splits[12], 1), 1, CTX).astype(jnp.int32)
    return dict(span_queries=span_queries, span_keys=span_keys, span_values=span_values, prefix_keys=prefix_keys, prefix_values=prefix_values, prefix_lengths=prefix_lengths, decode_queries=decode_queries, decode_new_keys=decode_new_keys, decode_new_values=decode_new_values, decode_key_cache=decode_key_cache, decode_value_cache=decode_value_cache, owner_map=owner_map, decode_lengths=decode_lengths)


def attend(queries, key_rows, value_rows, allowed):
    tokens = queries.shape[0]
    grouped = queries.reshape(tokens, KVH, H // KVH, HD).astype(jnp.float32)
    scores = jnp.einsum("tkgd,skd->tkgs", grouped, key_rows.astype(jnp.float32)) * (HD ** -0.5)
    visible = allowed[:, None, None, :]
    scores = jnp.where(visible, scores, -1.0e30)
    running_max = jnp.max(scores, axis=-1, keepdims=True)
    weights = jnp.where(visible, jnp.exp(scores - running_max), 0.0)
    normalizer = jnp.sum(weights, axis=-1)
    rounded = lax.optimization_barrier(weights.astype(jnp.bfloat16)).astype(jnp.float32)
    mixed = jnp.einsum("tkgs,skd->tkgd", rounded, value_rows.astype(jnp.float32))
    return (mixed / normalizer[..., None]).reshape(tokens, H, HD).astype(jnp.bfloat16)


def reference(span_queries, span_keys, span_values, prefix_keys, prefix_values, prefix_lengths, decode_queries, decode_new_keys, decode_new_values, decode_key_cache, decode_value_cache, owner_map, decode_lengths):
    position = jnp.arange(PREFIX, dtype=jnp.int32)
    prefix_live = (position % PRE_DEV) < prefix_lengths[position // PRE_DEV]
    all_keys = jnp.concatenate([prefix_keys, span_keys], axis=0)
    all_values = jnp.concatenate([prefix_values, span_values], axis=0)
    span_position = jnp.arange(SPAN, dtype=jnp.int32)

    def one_block(block_index):
        queries = lax.dynamic_slice_in_dim(span_queries, block_index * CH_DEV, CH_DEV)
        token_index = block_index * CH_DEV + jnp.arange(CH_DEV, dtype=jnp.int32)
        causal = span_position[None, :] <= token_index[:, None]
        allowed = jnp.concatenate([jnp.broadcast_to(prefix_live[None, :], (CH_DEV, PREFIX)), causal], axis=1)
        return attend(queries, all_keys, all_values, allowed)

    blocks = lax.map(one_block, jnp.arange(N_SEQ, dtype=jnp.int32))
    prefill_out = blocks.reshape(SPAN, H, HD)

    owners = owner_map[:, 0]
    order = jnp.arange(REQS, dtype=jnp.int32)
    earlier = (owners[None, :] == owners[:, None]) & (order[None, :] < order[:, None])
    ranking = jnp.sum(earlier.astype(jnp.int32), axis=1)
    slot_index = (owners * SLOTS + ranking).astype(jnp.int32)
    context_index = jnp.arange(CTX, dtype=jnp.int32)

    def one_request(items):
        query, new_key, new_value, length, slot = items
        cached_keys = lax.dynamic_index_in_dim(decode_key_cache, slot, 0, keepdims=False)
        cached_values = lax.dynamic_index_in_dim(decode_value_cache, slot, 0, keepdims=False)
        key_rows = jnp.concatenate([cached_keys, new_key[None]], axis=0)
        value_rows = jnp.concatenate([cached_values, new_value[None]], axis=0)
        allowed = jnp.concatenate([context_index < length, jnp.ones((1,), dtype=bool)])
        return attend(query[None], key_rows, value_rows, allowed[None])[0]

    outputs = lax.map(one_request, (decode_queries, decode_new_keys, decode_new_values, decode_lengths, slot_index))
    decode_out = jnp.zeros((OWN, H, HD), jnp.bfloat16).at[slot_index].set(outputs)
    return prefill_out, decode_out
```

```python
import math

import jax
import jax.numpy as jnp
from jax import lax
from jax.experimental import pallas as pl
from jax.experimental.pallas import tpu as pltpu
from jax.sharding import PartitionSpec as P

LOWEST = -1e30
FAR_AWAY = 1 << 30
PIECES = 8


def lookup_small(table, wanted):
    columns = jnp.arange(table.shape[0], dtype=jnp.int32)
    return jnp.sum(jnp.where(wanted[:, None] == columns[None, :], table[None, :], 0), axis=1)


def block_split(length):
    blocks = 1
    while length // blocks > 512 or length % blocks != 0:
        blocks += 1
    return blocks


def online_step(carried, queries, key_rows, value_rows, allowed):
    running_max, normalizer, weighted = carried
    scale = queries.shape[-1] ** (-0.5)
    scores = (
        jnp.einsum("tkgd,nkd->tkgn", queries, key_rows, preferred_element_type=jnp.float32) * scale
    )
    visible = allowed[:, None, None, :]
    scores = jnp.where(visible, scores, LOWEST)
    new_max = jnp.maximum(running_max, jnp.max(scores, axis=-1))
    weights = jnp.where(visible, jnp.exp(scores - new_max[..., None]), 0.0)
    factor = jnp.exp(running_max - new_max)
    normalizer = normalizer * factor + jnp.sum(weights, axis=-1)
    weighted = weighted * factor[..., None] + jnp.einsum(
        "tkgn,nkd->tkgd",
        weights.astype(jnp.bfloat16),
        value_rows,
        preferred_element_type=jnp.float32,
    )
    return (new_max, normalizer, weighted)


def guarded_step(carried, queries, key_rows, value_rows, allowed):
    return lax.cond(
        jnp.any(allowed),
        lambda inner: online_step(inner, queries, key_rows, value_rows, allowed),
        lambda inner: inner,
        carried,
    )


def fold_rows(carried, queries, key_rows, value_rows, allowed):
    length = key_rows.shape[0]
    blocks = block_split(length)
    if blocks == 1:
        return guarded_step(carried, queries, key_rows, value_rows, allowed)
    width = length // blocks
    stacked = (
        key_rows.reshape((blocks, width) + key_rows.shape[1:]),
        value_rows.reshape((blocks, width) + value_rows.shape[1:]),
        allowed.reshape(allowed.shape[0], blocks, width).transpose(1, 0, 2),
    )

    def visit(inner_carry, parts):
        return (guarded_step(inner_carry, queries, parts[0], parts[1], parts[2]), None)

    carried, unused = lax.scan(visit, carried, stacked)
    return carried


def on_large(
    span_queries,
    span_keys,
    span_values,
    prefix_keys,
    prefix_values,
    prefix_lengths,
    decode_queries,
    decode_new_keys,
    decode_new_values,
    decode_key_cache,
    decode_value_cache,
    owner_map,
    decode_lengths,
):
    device = lax.axis_index("seq")
    tokens_here, heads_here, head_dim = span_queries.shape
    kv_here = span_keys.shape[1]
    group_size = heads_here // kv_here
    queries = span_queries.reshape(tokens_here, kv_here, group_size, head_dim)
    token_index = device * tokens_here + jnp.arange(tokens_here, dtype=jnp.int32)
    prefix_here = prefix_keys.shape[0]
    initial = (
        jnp.full((tokens_here, kv_here, group_size), LOWEST, jnp.float32),
        jnp.zeros((tokens_here, kv_here, group_size), jnp.float32),
        jnp.zeros((tokens_here, kv_here, group_size, head_dim), jnp.float32),
    )
    stride = prefix_here + tokens_here
    both_keys = jnp.concatenate([prefix_keys, span_keys], axis=0)
    both_values = jnp.concatenate([prefix_values, span_values], axis=0)
    carried = initial
    key_rows = lax.all_gather(both_keys, "seq", axis=0, tiled=True)
    value_rows = lax.all_gather(both_values, "seq", axis=0, tiled=True)
    length = key_rows.shape[0]
    shards = length // stride
    tail = key_rows.shape[1:]
    keys_split = key_rows.reshape((shards, stride) + tail)
    values_split = value_rows.reshape((shards, stride) + tail)
    prefix_k = keys_split[:, :prefix_here].reshape((shards * prefix_here,) + tail)
    prefix_v = values_split[:, :prefix_here].reshape((shards * prefix_here,) + tail)
    span_k = keys_split[:, prefix_here:].reshape((shards * tokens_here,) + tail)
    span_v = values_split[:, prefix_here:].reshape((shards * tokens_here,) + tail)
    prefix_position = jnp.arange(shards * prefix_here, dtype=jnp.int32)
    prefix_ok = prefix_position % prefix_here < lookup_small(
        prefix_lengths, prefix_position // prefix_here
    )
    carried = fold_rows(
        carried,
        queries,
        prefix_k,
        prefix_v,
        jnp.broadcast_to(prefix_ok[None, :], (tokens_here, prefix_k.shape[0])),
    )
    span_position = jnp.arange(shards * tokens_here, dtype=jnp.int32)
    carried = fold_rows(
        carried, queries, span_k, span_v, span_position[None, :] <= token_index[:, None]
    )
    running_max, normalizer, weighted = carried
    prefill_out = (
        (weighted / normalizer[..., None])
        .reshape(tokens_here, heads_here, head_dim)
        .astype(jnp.bfloat16)
    )
    owners = owner_map[:, 0]
    requests = owners.shape[0]
    order = jnp.arange(requests, dtype=jnp.int32)
    earlier = (owners[None, :] == owners[:, None]) & (order[None, :] < order[:, None])
    ranking = jnp.sum(earlier.astype(jnp.int32), axis=1)
    slots_here = decode_key_cache.shape[0]
    slot_ids = jnp.arange(slots_here, dtype=jnp.int32)
    query_rows = lax.all_gather(decode_queries, "seq", axis=0, tiled=True)
    new_keys = lax.all_gather(decode_new_keys, "seq", axis=0, tiled=True)
    new_values = lax.all_gather(decode_new_values, "seq", axis=0, tiled=True)
    chosen = (owners == device)[None, :] & (ranking[None, :] == slot_ids[:, None])
    selector = chosen.astype(jnp.bfloat16)
    picked_queries = jnp.einsum(
        "sn,nhd->shd", selector, query_rows, preferred_element_type=jnp.float32
    )
    picked_keys = jnp.einsum("sn,nkd->skd", selector, new_keys, preferred_element_type=jnp.float32)
    picked_values = jnp.einsum(
        "sn,nkd->skd", selector, new_values, preferred_element_type=jnp.float32
    )
    picked_lengths = jnp.sum(jnp.where(chosen, decode_lengths[None, :], 0), axis=1)
    context = decode_key_cache.shape[1]
    grouped = picked_queries.astype(jnp.bfloat16).reshape(slots_here, kv_here, group_size, head_dim)
    own_keys = picked_keys.astype(jnp.bfloat16)
    own_values = picked_values.astype(jnp.bfloat16)
    scale = head_dim ** (-0.5)
    scores = (
        jnp.einsum("skgd,sckd->skgc", grouped, decode_key_cache, preferred_element_type=jnp.float32)
        * scale
    )
    visible = (jnp.arange(context, dtype=jnp.int32)[None, :] < picked_lengths[:, None])[
        :, None, None, :
    ]
    scores = jnp.where(visible, scores, LOWEST)
    own_score = (
        jnp.einsum("skgd,skd->skg", grouped, own_keys, preferred_element_type=jnp.float32) * scale
    )
    top_score = jnp.maximum(jnp.max(scores, axis=-1), own_score)
    weights = jnp.where(visible, jnp.exp(scores - top_score[..., None]), 0.0)
    own_weight = jnp.exp(own_score - top_score)
    total_weight = jnp.sum(weights, axis=-1) + own_weight
    rounded_own = lax.optimization_barrier(own_weight.astype(jnp.bfloat16)).astype(jnp.float32)
    mixed = jnp.einsum(
        "skgc,sckd->skgd",
        weights.astype(jnp.bfloat16),
        decode_value_cache,
        preferred_element_type=jnp.float32,
    )
    mixed = mixed + rounded_own[..., None] * own_values.astype(jnp.float32)[:, :, None, :]
    count_here = jnp.sum((owners == device).astype(jnp.int32))
    used = (slot_ids < count_here)[:, None, None, None]
    decode_out = (
        jnp.where(used, mixed / total_weight[..., None], 0.0)
        .reshape(slots_here, heads_here, head_dim)
        .astype(jnp.bfloat16)
    )
    return (prefill_out, decode_out)


class Sizes:
    def __init__(self, group, span_queries, span_keys, prefix_keys, decode_queries, cache):
        self.n = group
        self.half = group // 2
        self.tokens, self.heads, self.dim = span_queries.shape
        self.kv = span_keys.shape[1]
        self.share = self.heads // self.kv
        self.rows = self.tokens * self.heads
        self.pre = prefix_keys.shape[0]
        self.pre_rows = self.pre * self.kv
        self.block = self.pre_rows + self.tokens * self.kv
        self.cols = self.half * self.block
        self.asks = decode_queries.shape[0]
        self.ask_at = 2 * self.block
        self.new_at = self.ask_at + self.asks * self.heads
        self.new_rows = 2 * self.asks * self.kv
        self.pack = self.new_at + self.new_rows
        self.slots, self.context = cache.shape[:2]
        self.cache_rows = self.context * self.kv
        self.stat_rows = PIECES * self.rows // self.dim
        self.sel_at = self.rows + self.stat_rows
        self.sel_new_at = self.sel_at + self.slots * self.heads
        self.back = self.sel_new_at + self.slots * self.new_rows
        self.factor = self.dim**-0.5 * math.log2(math.e)

    def fits(self):
        power = self.n & (self.n - 1) == 0 and self.kv & (self.kv - 1) == 0
        return (
            power
            and 4 <= self.n <= 8
            and self.dim == 128
            and self.rows % 128 == 0
            and self.share % 16 == 0
            and self.block % 16 == 0
            and self.cols % 128 == 0
            and self.cache_rows % 128 == 0
            and self.new_rows == 8
        )


def column_tokens(z, me, lengths):
    column = lax.broadcasted_iota(jnp.int32, (8, z.cols), 1)
    block = jnp.zeros((8, z.cols), jnp.int32)
    for j in range(1, z.half):
        block = block + (column >= z.block * j).astype(jnp.int32)
    within = column - block * z.block
    live = jnp.full((8, z.cols), lengths[me], jnp.int32)
    first = jnp.full((8, z.cols), me * z.tokens, jnp.int32)
    for j in range(1, z.half):
        live = jnp.where(block == j, lengths[me ^ j], live)
        first = jnp.where(block == j, (me ^ j) * z.tokens, first)
    place = within >> (z.kv.bit_length() - 1)
    token = jnp.where(
        within < z.pre_rows,
        jnp.where(place < live, -1, FAR_AWAY),
        first + place - z.pre,
    )
    head = within & (z.kv - 1)
    return [jnp.where(head == h, token, FAR_AWAY) for h in range(z.kv)]


def partial_attention(z, me, whose, query, near, lengths, score_ref, weight_ref, top_ref, sum_ref):
    keys = jnp.concatenate([b[0 : z.block, :] for b in near], axis=0)
    score_ref[...] = lax.dot_general(
        query[...], keys, (((1,), (1,)), ((), ())), preferred_element_type=jnp.float32
    )
    tokens = column_tokens(z, me, lengths)
    for t in range(z.tokens):
        for h in range(z.kv):
            at = t * z.heads + h * z.share
            seen = tokens[h] <= whose * z.tokens + t
            scores = score_ref[at : at + z.share, :].reshape(z.share // 8, 8, z.cols)
            scores = jnp.where(seen[None], scores, LOWEST)
            top = jnp.max(scores, axis=-1, keepdims=True)
            weights = jnp.exp2((scores - top) * z.factor)
            top_ref[at : at + z.share, :] = top.reshape(z.share, 1)
            sum_ref[at : at + z.share, :] = jnp.sum(weights, axis=-1, keepdims=True).reshape(
                z.share, 1
            )
            weight_ref[at : at + z.share, :] = weights.reshape(z.share, z.cols).astype(jnp.bfloat16)
    values = jnp.concatenate([b[z.block : 2 * z.block, :] for b in near], axis=0)
    return jnp.dot(weight_ref[...], values, preferred_element_type=jnp.float32)


def route(z, owners, who, table):
    def visit(r, count):
        mine = owners[r] == who

        @pl.when(mine)
        def _():
            table[count] = r

        return count + mine.astype(jnp.int32)

    for s in range(z.slots):
        table[s] = -1
    lax.fori_loop(0, z.n * z.asks, visit, jnp.int32(0))


def pick_near(z, me, near, request):
    ask = jnp.zeros((z.heads, z.dim), jnp.bfloat16)
    new = jnp.zeros((z.new_rows, z.dim), jnp.bfloat16)
    for j in range(z.half):
        for a in range(z.asks):
            hit = request == (me ^ j) * z.asks + a
            at = z.ask_at + a * z.heads
            ask = jnp.where(hit, near[j][at : at + z.heads, :], ask)
            if a == 0:
                new = jnp.where(
                    (request >= 0) & (lax.div(request, z.asks) == (me ^ j)),
                    near[j][z.new_at : z.pack, :],
                    new,
                )
    return ask, new


def pieces_of(x):
    first = x.astype(jnp.bfloat16).astype(jnp.float32)
    second = (x - first).astype(jnp.bfloat16).astype(jnp.float32)
    third = (x - first - second).astype(jnp.bfloat16).astype(jnp.float32)
    return [first, second, third]


def far_kernel(z):
    def body(owners, lengths, query, *refs):
        near, (back, mine), scratch = refs[: z.half], refs[z.half : z.half + 2], refs[z.half + 2 :]
        score_ref, weight_ref, top_ref, sum_ref, table = scratch
        me = lax.axis_index("seq")
        partner = me ^ z.half
        for who, out, ask_at, new_at in (
            (partner, back, z.sel_at, z.sel_new_at),
            (me, mine, 0, z.slots * z.heads),
        ):
            route(z, owners, who, table)
            for s in range(z.slots):
                ask, new = pick_near(z, me, near, table[s])
                out[ask_at + s * z.heads : ask_at + (s + 1) * z.heads, :] = ask
                out[new_at + s * z.new_rows : new_at + (s + 1) * z.new_rows, :] = new
        mixed = partial_attention(
            z, me, partner, query, near, lengths, score_ref, weight_ref, top_ref, sum_ref
        )
        total = sum_ref[...]
        back[0 : z.rows, :] = (mixed / total).astype(jnp.bfloat16)
        lane = lax.broadcasted_iota(jnp.int32, (z.rows, z.dim), 1)
        packed = jnp.zeros((z.rows, z.dim), jnp.float32)
        for i, piece in enumerate(pieces_of(top_ref[...]) + pieces_of(total)):
            packed = jnp.where(lane == i, piece, packed)
        turned = jnp.transpose(packed)
        for i in range(z.rows // z.dim):
            back[z.rows + PIECES * i : z.rows + PIECES * (i + 1), :] = turned[
                :PIECES, i * z.dim : (i + 1) * z.dim
            ].astype(jnp.bfloat16)

    return body


def own_kernel(z):
    def body(lengths, query, *refs):
        near, (mixed, top_ref, sum_ref), (score_ref, weight_ref) = (
            refs[: z.half],
            refs[z.half : z.half + 3],
            refs[z.half + 3 :],
        )
        me = lax.axis_index("seq")
        mixed[...] = partial_attention(
            z, me, me, query, near, lengths, score_ref, weight_ref, top_ref, sum_ref
        )

    return body


def last_kernel(z):
    def body(
        owners, lengths, mixed, top_ref, sum_ref, mine, back, keys, values, out, decoded, table
    ):
        me = lax.axis_index("seq")
        route(z, owners, me, table)
        turned = jnp.concatenate(
            [
                back[z.rows + PIECES * i : z.rows + PIECES * (i + 1), :].astype(jnp.float32)
                for i in range(z.rows // z.dim)
            ],
            axis=1,
        )
        packed = jnp.transpose(
            jnp.concatenate([turned, jnp.zeros((z.dim - PIECES, z.rows), jnp.float32)], axis=0)
        )
        far_top = packed[:, 0:1] + packed[:, 1:2] + packed[:, 2:3]
        far_sum = packed[:, 3:4] + packed[:, 4:5] + packed[:, 5:6]
        top = jnp.maximum(top_ref[...], far_top)
        here = jnp.exp2((top_ref[...] - top) * z.factor)
        there = jnp.exp2((far_top - top) * z.factor) * far_sum
        joined = mixed[...] * here + back[0 : z.rows, :].astype(jnp.float32) * there
        out[...] = (joined / (sum_ref[...] * here + there)).astype(jnp.bfloat16)

        column = lax.broadcasted_iota(jnp.int32, (z.heads, z.cache_rows), 1)
        row = lax.broadcasted_iota(jnp.int32, (z.heads, z.cache_rows), 0)
        shift = z.share.bit_length() - 1
        match = (column & (z.kv - 1)) == (row >> shift)
        place = column >> (z.kv.bit_length() - 1)
        head_of = lax.broadcasted_iota(jnp.int32, (z.heads, z.dim), 0) >> shift
        for s in range(z.slots):
            request = table[s]
            used = request >= 0
            safe = jnp.maximum(request, 0)
            source = lax.div(safe, z.asks)
            at = safe - source * z.asks
            from_far = (source ^ me) >= z.half
            ask = jnp.where(
                from_far,
                back[z.sel_at + s * z.heads : z.sel_at + (s + 1) * z.heads, :],
                mine[s * z.heads : (s + 1) * z.heads, :],
            )
            first = z.slots * z.heads
            new = jnp.where(
                from_far,
                back[z.sel_new_at + s * z.new_rows : z.sel_new_at + (s + 1) * z.new_rows, :],
                mine[first + s * z.new_rows : first + (s + 1) * z.new_rows, :],
            ).astype(jnp.float32)
            new_key = jnp.zeros((z.heads, z.dim), jnp.float32)
            new_value = jnp.zeros((z.heads, z.dim), jnp.float32)
            for a in range(z.asks):
                for h in range(z.kv):
                    here_now = (head_of == h) & (at == a)
                    i = a * z.kv + h
                    new_key = jnp.where(here_now, new[i : i + 1, :], new_key)
                    i = i + z.asks * z.kv
                    new_value = jnp.where(here_now, new[i : i + 1, :], new_value)
            scores = lax.dot_general(
                ask,
                keys[s * z.cache_rows : (s + 1) * z.cache_rows, :],
                (((1,), (1,)), ((), ())),
                preferred_element_type=jnp.float32,
            )
            own = jnp.sum(ask.astype(jnp.float32) * new_key, axis=-1, keepdims=True)
            scores = jnp.where(match & (place < lengths[safe]), scores, LOWEST)
            peak = jnp.maximum(jnp.max(scores, axis=-1, keepdims=True), own)
            weights = jnp.exp2((scores - peak) * z.factor)
            own_weight = jnp.exp2((own - peak) * z.factor)
            total = jnp.sum(weights, axis=-1, keepdims=True) + own_weight
            result = jnp.dot(
                weights.astype(jnp.bfloat16),
                values[s * z.cache_rows : (s + 1) * z.cache_rows, :],
                preferred_element_type=jnp.float32,
            )
            result = result + own_weight.astype(jnp.bfloat16).astype(jnp.float32) * new_value
            decoded[s * z.heads : (s + 1) * z.heads, :] = jnp.where(
                used, result / total, 0.0
            ).astype(jnp.bfloat16)

    return body


def swap(x, n, by):
    return lax.ppermute(x, "seq", [(i, i ^ by) for i in range(n)])


def on_small(
    z,
    span_queries,
    span_keys,
    span_values,
    prefix_keys,
    prefix_values,
    prefix_lengths,
    decode_queries,
    decode_new_keys,
    decode_new_values,
    decode_key_cache,
    decode_value_cache,
    owner_map,
    decode_lengths,
):
    def flat(x):
        return x.reshape(-1, z.dim)

    smem = pl.BlockSpec(memory_space=pltpu.SMEM)
    vmem = pl.BlockSpec(memory_space=pltpu.VMEM)
    queries = flat(span_queries)
    owners = owner_map.reshape(-1)
    far_queries = swap(queries, z.n, z.half)
    packed = jnp.concatenate(
        [
            flat(prefix_keys),
            flat(span_keys),
            flat(prefix_values),
            flat(span_values),
            flat(decode_queries),
            flat(decode_new_keys),
            flat(decode_new_values),
        ],
        axis=0,
    )
    near = [packed] + [swap(packed, z.n, j) for j in range(1, z.half)]
    wide = [pltpu.VMEM((z.rows, z.cols), jnp.float32), pltpu.VMEM((z.rows, z.cols), jnp.bfloat16)]
    thin = jax.ShapeDtypeStruct((z.rows, 1), jnp.float32)
    thin_scratch = pltpu.VMEM((z.rows, 1), jnp.float32)
    sent, mine = pl.pallas_call(
        far_kernel(z),
        out_shape=[
            jax.ShapeDtypeStruct((z.back, z.dim), jnp.bfloat16),
            jax.ShapeDtypeStruct((z.slots * (z.heads + z.new_rows), z.dim), jnp.bfloat16),
        ],
        in_specs=[smem, smem] + [vmem] * (1 + z.half),
        out_specs=[vmem, vmem],
        scratch_shapes=wide
        + [thin_scratch, thin_scratch, pltpu.SMEM((z.slots,), jnp.int32)],
        name="far_part",
    )(owners, prefix_lengths, far_queries, *near)
    back = swap(sent, z.n, z.half)
    mixed, top, total = pl.pallas_call(
        own_kernel(z),
        out_shape=[jax.ShapeDtypeStruct((z.rows, z.dim), jnp.float32), thin, thin],
        in_specs=[smem] + [vmem] * (1 + z.half),
        out_specs=[vmem] * 3,
        scratch_shapes=wide,
        name="own_part",
    )(prefix_lengths, queries, *near)
    out, decoded = pl.pallas_call(
        last_kernel(z),
        out_shape=[
            jax.ShapeDtypeStruct((z.rows, z.dim), jnp.bfloat16),
            jax.ShapeDtypeStruct((z.slots * z.heads, z.dim), jnp.bfloat16),
        ],
        in_specs=[smem, smem] + [vmem] * 7,
        out_specs=[vmem, vmem],
        scratch_shapes=[pltpu.SMEM((z.slots,), jnp.int32)],
        name="last_part",
    )(
        owners,
        decode_lengths,
        mixed,
        top,
        total,
        mine,
        back,
        flat(decode_key_cache),
        flat(decode_value_cache),
    )
    return (
        out.reshape(z.tokens, z.heads, z.dim),
        decoded.reshape(z.slots, z.heads, z.dim),
    )


def solution(mesh):
    group = mesh.shape["seq"]

    def on_device(*args):
        z = Sizes(group, args[0], args[1], args[3], args[6], args[9])
        if z.fits():
            return on_small(z, *args)
        return on_large(*args)

    return jax.shard_map(
        on_device,
        mesh=mesh,
        in_specs=(
            P(("groups", "seq"), "tp", None),
            P(("groups", "seq"), "tp", None),
            P(("groups", "seq"), "tp", None),
            P(("groups", "seq"), "tp", None),
            P(("groups", "seq"), "tp", None),
            P("groups"),
            P(("groups", "seq"), "tp", None),
            P(("groups", "seq"), "tp", None),
            P(("groups", "seq"), "tp", None),
            P(("groups", "seq"), None, "tp", None),
            P(("groups", "seq"), None, "tp", None),
            P("groups", None),
            P("groups"),
        ),
        out_specs=(P(("groups", "seq"), "tp", None), P(("groups", "seq"), "tp", None)),
        check_vma=False,
    )
```

```python
import math

import jax
import jax.numpy as jnp
from jax import lax
from jax.experimental import pallas as pl
from jax.experimental.pallas import tpu as pltpu
from jax.sharding import PartitionSpec as P


LOWEST = -1e30
FAR_AWAY = 1 << 30
PIECES = 8


def lookup_small(table, wanted):
    columns = jnp.arange(table.shape[0], dtype=jnp.int32)
    return jnp.sum(jnp.where(wanted[:, None] == columns[None, :], table[None, :], 0), axis=1)


def block_split(length):
    blocks = 1
    while length // blocks > 512 or length % blocks != 0:
        blocks += 1
    return blocks


def online_step(carried, queries, key_rows, value_rows, allowed):
    running_max, normalizer, weighted = carried
    scale = queries.shape[-1] ** (-0.5)
    scores = (
        jnp.einsum("tkgd,nkd->tkgn", queries, key_rows, preferred_element_type=jnp.float32) * scale
    )
    visible = allowed[:, None, None, :]
    scores = jnp.where(visible, scores, LOWEST)
    new_max = jnp.maximum(running_max, jnp.max(scores, axis=-1))
    weights = jnp.where(visible, jnp.exp(scores - new_max[..., None]), 0.0)
    factor = jnp.exp(running_max - new_max)
    normalizer = normalizer * factor + jnp.sum(weights, axis=-1)
    weighted = weighted * factor[..., None] + jnp.einsum(
        "tkgn,nkd->tkgd",
        weights.astype(jnp.bfloat16),
        value_rows,
        preferred_element_type=jnp.float32,
    )
    return (new_max, normalizer, weighted)


def guarded_step(carried, queries, key_rows, value_rows, allowed):
    return lax.cond(
        jnp.any(allowed),
        lambda inner: online_step(inner, queries, key_rows, value_rows, allowed),
        lambda inner: inner,
        carried,
    )


def fold_rows(carried, queries, key_rows, value_rows, allowed):
    length = key_rows.shape[0]
    blocks = block_split(length)
    if blocks == 1:
        return guarded_step(carried, queries, key_rows, value_rows, allowed)
    width = length // blocks
    stacked = (
        key_rows.reshape((blocks, width) + key_rows.shape[1:]),
        value_rows.reshape((blocks, width) + value_rows.shape[1:]),
        allowed.reshape(allowed.shape[0], blocks, width).transpose(1, 0, 2),
    )

    def visit(inner_carry, parts):
        return (guarded_step(inner_carry, queries, parts[0], parts[1], parts[2]), None)

    carried, _ = lax.scan(visit, carried, stacked)
    return carried


def on_large(
    span_queries,
    span_keys,
    span_values,
    prefix_keys,
    prefix_values,
    prefix_lengths,
    decode_queries,
    decode_new_keys,
    decode_new_values,
    decode_key_cache,
    decode_value_cache,
    owner_map,
    decode_lengths,
):
    device = lax.axis_index("seq")
    tokens_here, heads_here, head_dim = span_queries.shape
    kv_here = span_keys.shape[1]
    group_size = heads_here // kv_here
    queries = span_queries.reshape(tokens_here, kv_here, group_size, head_dim)
    token_index = device * tokens_here + jnp.arange(tokens_here, dtype=jnp.int32)
    prefix_here = prefix_keys.shape[0]
    initial = (
        jnp.full((tokens_here, kv_here, group_size), LOWEST, jnp.float32),
        jnp.zeros((tokens_here, kv_here, group_size), jnp.float32),
        jnp.zeros((tokens_here, kv_here, group_size, head_dim), jnp.float32),
    )
    stride = prefix_here + tokens_here
    both_keys = jnp.concatenate([prefix_keys, span_keys], axis=0)
    both_values = jnp.concatenate([prefix_values, span_values], axis=0)
    carried = initial
    key_rows = lax.all_gather(both_keys, "seq", axis=0, tiled=True)
    value_rows = lax.all_gather(both_values, "seq", axis=0, tiled=True)
    length = key_rows.shape[0]
    shards = length // stride
    tail = key_rows.shape[1:]
    keys_split = key_rows.reshape((shards, stride) + tail)
    values_split = value_rows.reshape((shards, stride) + tail)
    prefix_k = keys_split[:, :prefix_here].reshape((shards * prefix_here,) + tail)
    prefix_v = values_split[:, :prefix_here].reshape((shards * prefix_here,) + tail)
    span_k = keys_split[:, prefix_here:].reshape((shards * tokens_here,) + tail)
    span_v = values_split[:, prefix_here:].reshape((shards * tokens_here,) + tail)
    prefix_position = jnp.arange(shards * prefix_here, dtype=jnp.int32)
    prefix_ok = prefix_position % prefix_here < lookup_small(
        prefix_lengths, prefix_position // prefix_here
    )
    carried = fold_rows(
        carried,
        queries,
        prefix_k,
        prefix_v,
        jnp.broadcast_to(prefix_ok[None, :], (tokens_here, prefix_k.shape[0])),
    )
    span_position = jnp.arange(shards * tokens_here, dtype=jnp.int32)
    carried = fold_rows(
        carried, queries, span_k, span_v, span_position[None, :] <= token_index[:, None]
    )
    _, normalizer, weighted = carried
    prefill_out = (
        (weighted / normalizer[..., None])
        .reshape(tokens_here, heads_here, head_dim)
        .astype(jnp.bfloat16)
    )
    owners = owner_map[:, 0]
    requests = owners.shape[0]
    order = jnp.arange(requests, dtype=jnp.int32)
    earlier = (owners[None, :] == owners[:, None]) & (order[None, :] < order[:, None])
    ranking = jnp.sum(earlier.astype(jnp.int32), axis=1)
    slots_here = decode_key_cache.shape[0]
    slot_ids = jnp.arange(slots_here, dtype=jnp.int32)
    query_rows = lax.all_gather(decode_queries, "seq", axis=0, tiled=True)
    new_keys = lax.all_gather(decode_new_keys, "seq", axis=0, tiled=True)
    new_values = lax.all_gather(decode_new_values, "seq", axis=0, tiled=True)
    chosen = (owners == device)[None, :] & (ranking[None, :] == slot_ids[:, None])
    selector = chosen.astype(jnp.bfloat16)
    picked_queries = jnp.einsum(
        "sn,nhd->shd", selector, query_rows, preferred_element_type=jnp.float32
    )
    picked_keys = jnp.einsum("sn,nkd->skd", selector, new_keys, preferred_element_type=jnp.float32)
    picked_values = jnp.einsum(
        "sn,nkd->skd", selector, new_values, preferred_element_type=jnp.float32
    )
    picked_lengths = jnp.sum(jnp.where(chosen, decode_lengths[None, :], 0), axis=1)
    context = decode_key_cache.shape[1]
    grouped = picked_queries.astype(jnp.bfloat16).reshape(slots_here, kv_here, group_size, head_dim)
    own_keys = picked_keys.astype(jnp.bfloat16)
    own_values = picked_values.astype(jnp.bfloat16)
    scale = head_dim ** (-0.5)
    scores = (
        jnp.einsum("skgd,sckd->skgc", grouped, decode_key_cache, preferred_element_type=jnp.float32)
        * scale
    )
    visible = (jnp.arange(context, dtype=jnp.int32)[None, :] < picked_lengths[:, None])[
        :, None, None, :
    ]
    scores = jnp.where(visible, scores, LOWEST)
    own_score = (
        jnp.einsum("skgd,skd->skg", grouped, own_keys, preferred_element_type=jnp.float32) * scale
    )
    top_score = jnp.maximum(jnp.max(scores, axis=-1), own_score)
    weights = jnp.where(visible, jnp.exp(scores - top_score[..., None]), 0.0)
    own_weight = jnp.exp(own_score - top_score)
    total_weight = jnp.sum(weights, axis=-1) + own_weight
    rounded_own = lax.optimization_barrier(own_weight.astype(jnp.bfloat16)).astype(jnp.float32)
    mixed = jnp.einsum(
        "skgc,sckd->skgd",
        weights.astype(jnp.bfloat16),
        decode_value_cache,
        preferred_element_type=jnp.float32,
    )
    mixed = mixed + rounded_own[..., None] * own_values.astype(jnp.float32)[:, :, None, :]
    count_here = jnp.sum((owners == device).astype(jnp.int32))
    used = (slot_ids < count_here)[:, None, None, None]
    decode_out = (
        jnp.where(used, mixed / total_weight[..., None], 0.0)
        .reshape(slots_here, heads_here, head_dim)
        .astype(jnp.bfloat16)
    )
    return (prefill_out, decode_out)


class Sizes:
    def __init__(self, group, span_queries, span_keys, prefix_keys, decode_queries, cache):
        self.n = group
        self.half = group // 2
        self.tokens, self.heads, self.dim = span_queries.shape
        self.kv = span_keys.shape[1]
        self.share = self.heads // self.kv
        self.rows = self.tokens * self.heads
        self.pre = prefix_keys.shape[0]
        self.pre_rows = self.pre * self.kv
        self.block = self.pre_rows + self.tokens * self.kv
        self.cols = self.half * self.block
        self.asks = decode_queries.shape[0]
        self.ask_at = 2 * self.block
        self.new_at = self.ask_at + self.asks * self.heads
        self.new_rows = 2 * self.asks * self.kv
        self.pack = self.new_at + self.new_rows
        self.slots, self.context = cache.shape[:2]
        self.cache_rows = self.context * self.kv
        self.stat_rows = PIECES * self.rows // self.dim
        self.sel_at = self.rows + self.stat_rows
        self.sel_new_at = self.sel_at + self.slots * self.heads
        self.back = self.sel_new_at + self.slots * self.new_rows
        self.factor = self.dim**-0.5 * math.log2(math.e)

    def fits(self):
        power = self.n & (self.n - 1) == 0 and self.kv & (self.kv - 1) == 0
        return (
            power
            and 4 <= self.n <= 8
            and self.dim == 128
            and self.rows % 128 == 0
            and self.share % 16 == 0
            and self.block % 16 == 0
            and self.cols % 128 == 0
            and self.cache_rows % 128 == 0
            and self.new_rows == 8
        )


def column_tokens(z, me, table):
    lengths = [table[3 * z.slots + (me ^ j)] for j in range(z.half)]
    column = lax.broadcasted_iota(jnp.int32, (8, z.cols), 1)
    block = jnp.zeros((8, z.cols), jnp.int32)
    for j in range(1, z.half):
        block = block + (column >= z.block * j).astype(jnp.int32)
    within = column - block * z.block
    live = jnp.full((8, z.cols), lengths[0], jnp.int32)
    first = jnp.full((8, z.cols), me * z.tokens, jnp.int32)
    for j in range(1, z.half):
        live = jnp.where(block == j, lengths[j], live)
        first = jnp.where(block == j, (me ^ j) * z.tokens, first)
    place = within >> (z.kv.bit_length() - 1)
    token = jnp.where(
        within < z.pre_rows,
        jnp.where(place < live, -1, FAR_AWAY),
        first + place - z.pre,
    )
    head = within & (z.kv - 1)
    return [jnp.where(head == h, token, FAR_AWAY) for h in range(z.kv)]


def partial_attention(z, me, whose, query, near, table, score_ref, weight_ref, top_ref, sum_ref):
    keys = jnp.concatenate([b[0 : z.block, :] for b in near], axis=0)
    score_ref[...] = lax.dot_general(
        query[...], keys, (((1,), (1,)), ((), ())), preferred_element_type=jnp.float32
    )
    tokens = column_tokens(z, me, table)
    for t in range(z.tokens):
        for h in range(z.kv):
            at = t * z.heads + h * z.share
            seen = tokens[h] <= whose * z.tokens + t
            scores = score_ref[at : at + z.share, :].reshape(z.share // 8, 8, z.cols)
            scores = jnp.where(seen[None], scores, LOWEST)
            top = jnp.max(scores, axis=-1, keepdims=True)
            weights = jnp.exp2((scores - top) * z.factor)
            top_ref[at : at + z.share, :] = top.reshape(z.share, 1)
            sum_ref[at : at + z.share, :] = jnp.sum(weights, axis=-1, keepdims=True).reshape(
                z.share, 1
            )
            weight_ref[at : at + z.share, :] = weights.reshape(z.share, z.cols).astype(jnp.bfloat16)
    values = jnp.concatenate([b[z.block : 2 * z.block, :] for b in near], axis=0)
    return jnp.dot(weight_ref[...], values, preferred_element_type=jnp.float32)


def plan_kernel(z):
    def body(owners, lengths, cached, table):
        me = lax.axis_index("seq")
        partner = me ^ z.half
        for i in range(2 * z.slots):
            table[i] = -1

        def visit(r, counts):
            mine = owners[r] == me
            theirs = owners[r] == partner

            @pl.when(mine)
            def _():
                table[counts[0]] = r
                table[2 * z.slots + counts[0]] = cached[r]

            @pl.when(theirs)
            def _():
                table[z.slots + counts[1]] = r

            return (counts[0] + mine.astype(jnp.int32), counts[1] + theirs.astype(jnp.int32))

        lax.fori_loop(0, z.n * z.asks, visit, (jnp.int32(0), jnp.int32(0)))
        for i in range(z.n):
            table[3 * z.slots + i] = lengths[i]

    return body


def pick_near(z, me, near, request):
    ask = jnp.zeros((z.heads, z.dim), jnp.bfloat16)
    new = jnp.zeros((z.new_rows, z.dim), jnp.bfloat16)
    for j in range(z.half):
        for a in range(z.asks):
            hit = request == (me ^ j) * z.asks + a
            at = z.ask_at + a * z.heads
            ask = jnp.where(hit, near[j][at : at + z.heads, :], ask)
            if a == 0:
                new = jnp.where(
                    (request >= 0) & (lax.div(request, z.asks) == (me ^ j)),
                    near[j][z.new_at : z.pack, :],
                    new,
                )
    return ask, new


def pieces_of(x):
    first = x.astype(jnp.bfloat16).astype(jnp.float32)
    second = (x - first).astype(jnp.bfloat16).astype(jnp.float32)
    third = (x - first - second).astype(jnp.bfloat16).astype(jnp.float32)
    return [first, second, third]


def pack_kernel(z):
    def body(*refs):
        out, new, sems = refs[-3:]
        copies, at = [], 0
        for i, ref in enumerate(refs[:7]):
            rows = ref.shape[0]
            into = out.at[pl.ds(at, rows), :] if i < 5 else new.at[i - 5]
            copies.append(pltpu.make_async_copy(ref, into, sems.at[i]))
            at += rows
        for copy in reversed(copies):
            copy.start()
        for copy in reversed(copies):
            copy.wait()
        both = [new[i].astype(jnp.float32) for i in range(2)]
        out[z.new_at : z.pack, :] = jnp.concatenate(both, axis=0).astype(jnp.bfloat16)

    return body


def far_kernel(z):
    def body(table, query, *refs):
        near, back, scratch = refs[: z.half], refs[z.half], refs[z.half + 1 :]
        score_ref, weight_ref, top_ref, sum_ref = scratch
        me = lax.axis_index("seq")
        for s in range(z.slots):
            ask, new = pick_near(z, me, near, table[z.slots + s])
            at = z.sel_at + s * z.heads
            back[at : at + z.heads, :] = ask
            at = z.sel_new_at + s * z.new_rows
            back[at : at + z.new_rows, :] = new
        mixed = partial_attention(
            z, me, me ^ z.half, query, near, table, score_ref, weight_ref, top_ref, sum_ref
        )
        total = sum_ref[...]
        back[0 : z.rows, :] = (mixed / total).astype(jnp.bfloat16)
        lane = lax.broadcasted_iota(jnp.int32, (z.rows, z.dim), 1)
        packed = jnp.zeros((z.rows, z.dim), jnp.float32)
        for i, piece in enumerate(pieces_of(top_ref[...]) + pieces_of(total)):
            packed = jnp.where(lane == i, piece, packed)
        turned = jnp.transpose(packed)
        for i in range(z.rows // z.dim):
            back[z.rows + PIECES * i : z.rows + PIECES * (i + 1), :] = turned[
                :PIECES, i * z.dim : (i + 1) * z.dim
            ].astype(jnp.bfloat16)

    return body


def own_kernel(z):
    def body(table, query, *refs):
        near, (mixed, top_ref, sum_ref, mine), (score_ref, weight_ref) = (
            refs[: z.half],
            refs[z.half : z.half + 4],
            refs[z.half + 4 :],
        )
        me = lax.axis_index("seq")
        for s in range(z.slots):
            ask, new = pick_near(z, me, near, table[s])
            mine[s * z.heads : (s + 1) * z.heads, :] = ask
            at = z.slots * z.heads + s * z.new_rows
            mine[at : at + z.new_rows, :] = new
        mixed[...] = partial_attention(
            z, me, me, query, near, table, score_ref, weight_ref, top_ref, sum_ref
        )

    return body


def last_kernel(z):
    def body(
        table, mixed, top_ref, sum_ref, mine, back, keys, values, *outs
    ):
        out_hbm, decoded_hbm, out, decoded, sems = outs
        me = lax.axis_index("seq")
        turned = jnp.concatenate(
            [
                back[z.rows + PIECES * i : z.rows + PIECES * (i + 1), :].astype(jnp.float32)
                for i in range(z.rows // z.dim)
            ],
            axis=1,
        )
        packed = jnp.transpose(
            jnp.concatenate([turned, jnp.zeros((z.dim - PIECES, z.rows), jnp.float32)], axis=0)
        )
        far_top = packed[:, 0:1] + packed[:, 1:2] + packed[:, 2:3]
        far_sum = packed[:, 3:4] + packed[:, 4:5] + packed[:, 5:6]
        top = jnp.maximum(top_ref[...], far_top)
        here = jnp.exp2((top_ref[...] - top) * z.factor)
        there = jnp.exp2((far_top - top) * z.factor) * far_sum
        joined = mixed[...] * here + back[0 : z.rows, :].astype(jnp.float32) * there
        out[...] = (joined / (sum_ref[...] * here + there)).astype(jnp.bfloat16)
        first_copy = pltpu.make_async_copy(out, out_hbm, sems.at[0])
        first_copy.start()

        column = lax.broadcasted_iota(jnp.int32, (z.heads, z.cache_rows), 1)
        row = lax.broadcasted_iota(jnp.int32, (z.heads, z.cache_rows), 0)
        shift = z.share.bit_length() - 1
        match = (column & (z.kv - 1)) == (row >> shift)
        place = column >> (z.kv.bit_length() - 1)
        head_of = lax.broadcasted_iota(jnp.int32, (z.heads, z.dim), 0) >> shift
        for s in range(z.slots):
            request = table[s]
            used = request >= 0
            safe = jnp.maximum(request, 0)
            source = lax.div(safe, z.asks)
            at = safe - source * z.asks
            from_far = (source ^ me) >= z.half
            ask = jnp.where(
                from_far,
                back[z.sel_at + s * z.heads : z.sel_at + (s + 1) * z.heads, :],
                mine[s * z.heads : (s + 1) * z.heads, :],
            )
            first = z.slots * z.heads
            new = jnp.where(
                from_far,
                back[z.sel_new_at + s * z.new_rows : z.sel_new_at + (s + 1) * z.new_rows, :],
                mine[first + s * z.new_rows : first + (s + 1) * z.new_rows, :],
            ).astype(jnp.float32)
            new_key = jnp.zeros((z.heads, z.dim), jnp.float32)
            new_value = jnp.zeros((z.heads, z.dim), jnp.float32)
            for a in range(z.asks):
                for h in range(z.kv):
                    here_now = (head_of == h) & (at == a)
                    i = a * z.kv + h
                    new_key = jnp.where(here_now, new[i : i + 1, :], new_key)
                    i = i + z.asks * z.kv
                    new_value = jnp.where(here_now, new[i : i + 1, :], new_value)
            scores = lax.dot_general(
                ask,
                keys[s * z.cache_rows : (s + 1) * z.cache_rows, :],
                (((1,), (1,)), ((), ())),
                preferred_element_type=jnp.float32,
            )
            own = jnp.sum(ask.astype(jnp.float32) * new_key, axis=-1, keepdims=True)
            scores = jnp.where(match & (place < table[2 * z.slots + s]), scores, LOWEST)
            peak = jnp.maximum(jnp.max(scores, axis=-1, keepdims=True), own)
            weights = jnp.exp2((scores - peak) * z.factor)
            own_weight = jnp.exp2((own - peak) * z.factor)
            total = jnp.sum(weights, axis=-1, keepdims=True) + own_weight
            result = jnp.dot(
                weights.astype(jnp.bfloat16),
                values[s * z.cache_rows : (s + 1) * z.cache_rows, :],
                preferred_element_type=jnp.float32,
            )
            result = result + own_weight.astype(jnp.bfloat16).astype(jnp.float32) * new_value
            decoded[s * z.heads : (s + 1) * z.heads, :] = jnp.where(
                used, result / total, 0.0
            ).astype(jnp.bfloat16)
        second_copy = pltpu.make_async_copy(decoded, decoded_hbm, sems.at[1])
        second_copy.start()
        first_copy.wait()
        second_copy.wait()

    return body


def swap(x, n, by):
    return lax.ppermute(x, "seq", [(i, i ^ by) for i in range(n)])


def on_small(
    z,
    span_queries,
    span_keys,
    span_values,
    prefix_keys,
    prefix_values,
    prefix_lengths,
    decode_queries,
    decode_new_keys,
    decode_new_values,
    decode_key_cache,
    decode_value_cache,
    owner_map,
    decode_lengths,
):
    def flat(x):
        return x.reshape(-1, z.dim)

    def local(x):
        return pltpu.with_memory_space_constraint(x, pltpu.VMEM)

    smem = pl.BlockSpec(memory_space=pltpu.SMEM)
    vmem = pl.BlockSpec(memory_space=pltpu.VMEM)
    hbm = pl.BlockSpec(memory_space=pl.ANY)

    def ints(x):
        return pltpu.with_memory_space_constraint(x, pltpu.SMEM)

    queries = flat(span_queries)
    far_queries = local(swap(queries, z.n, z.half))
    packed = pl.pallas_call(
        pack_kernel(z),
        out_shape=pltpu.VMEM((z.pack, z.dim), jnp.bfloat16),
        in_specs=[hbm] * 7,
        out_specs=vmem,
        scratch_shapes=[
            pltpu.VMEM((2, z.asks * z.kv, z.dim), jnp.bfloat16),
            pltpu.SemaphoreType.DMA((7,)),
        ],
        name="pack",
    )(
        flat(prefix_keys),
        flat(span_keys),
        flat(prefix_values),
        flat(span_values),
        flat(decode_queries),
        flat(decode_new_keys),
        flat(decode_new_values),
    )
    near = [local(packed)]
    for j in range(1, z.half):
        near.append(local(swap(packed, z.n, j)))
    table = pl.pallas_call(
        plan_kernel(z),
        out_shape=pltpu.SMEM((3 * z.slots + z.n,), jnp.int32),
        in_specs=[smem] * 3,
        out_specs=smem,
        name="plan",
    )(owner_map.reshape(-1), prefix_lengths, decode_lengths)
    table = ints(table)
    wide = [pltpu.VMEM((z.rows, z.cols), jnp.float32), pltpu.VMEM((z.rows, z.cols), jnp.bfloat16)]
    thin = pltpu.VMEM((z.rows, 1), jnp.float32)
    sent = pl.pallas_call(
        far_kernel(z),
        out_shape=pltpu.VMEM((z.back, z.dim), jnp.bfloat16),
        in_specs=[smem] + [vmem] * (1 + z.half),
        out_specs=vmem,
        scratch_shapes=wide + [thin, thin],
        name="far_part",
    )(table, far_queries, *near)
    back = local(swap(sent, z.n, z.half))
    held = pl.pallas_call(
        own_kernel(z),
        out_shape=[
            pltpu.VMEM((z.rows, z.dim), jnp.float32),
            thin,
            thin,
            pltpu.VMEM((z.slots * (z.heads + z.new_rows), z.dim), jnp.bfloat16),
        ],
        in_specs=[smem] + [vmem] * (1 + z.half),
        out_specs=[vmem] * 4,
        scratch_shapes=wide,
        name="own_part",
    )(table, local(queries), *near)
    out, decoded = pl.pallas_call(
        last_kernel(z),
        out_shape=[
            jax.ShapeDtypeStruct((z.rows, z.dim), jnp.bfloat16),
            jax.ShapeDtypeStruct((z.slots * z.heads, z.dim), jnp.bfloat16),
        ],
        in_specs=[smem] + [vmem] * 7,
        out_specs=[hbm, hbm],
        scratch_shapes=[
            pltpu.VMEM((z.rows, z.dim), jnp.bfloat16),
            pltpu.VMEM((z.slots * z.heads, z.dim), jnp.bfloat16),
            pltpu.SemaphoreType.DMA((2,)),
        ],
        name="last_part",
    )(
        table,
        *[local(x) for x in held],
        back,
        local(flat(decode_key_cache)),
        local(flat(decode_value_cache)),
    )
    return (
        out.reshape(z.tokens, z.heads, z.dim),
        decoded.reshape(z.slots, z.heads, z.dim),
    )


def solution(mesh):
    group = mesh.shape["seq"]

    def on_device(*args):
        z = Sizes(group, args[0], args[1], args[3], args[6], args[9])
        if z.fits():
            return on_small(z, *args)
        return on_large(*args)

    return jax.shard_map(
        on_device,
        mesh=mesh,
        in_specs=(
            P(("groups", "seq"), "tp", None),
            P(("groups", "seq"), "tp", None),
            P(("groups", "seq"), "tp", None),
            P(("groups", "seq"), "tp", None),
            P(("groups", "seq"), "tp", None),
            P("groups"),
            P(("groups", "seq"), "tp", None),
            P(("groups", "seq"), "tp", None),
            P(("groups", "seq"), "tp", None),
            P(("groups", "seq"), None, "tp", None),
            P(("groups", "seq"), None, "tp", None),
            P("groups", None),
            P("groups"),
        ),
        out_specs=(P(("groups", "seq"), "tp", None), P(("groups", "seq"), "tp", None)),
        check_vma=False,
    )
```

```python
import math

import jax
import jax.numpy as jnp
from jax import lax
from jax.experimental import pallas as pl
from jax.experimental.pallas import tpu as pltpu
from jax.sharding import PartitionSpec as P


LOWEST = -1e30
FAR_AWAY = 1 << 30
PIECES = 8


def lookup_small(table, wanted):
    columns = jnp.arange(table.shape[0], dtype=jnp.int32)
    return jnp.sum(jnp.where(wanted[:, None] == columns[None, :], table[None, :], 0), axis=1)


def block_split(length):
    blocks = 1
    while length // blocks > 512 or length % blocks != 0:
        blocks += 1
    return blocks


def online_step(carried, queries, key_rows, value_rows, allowed):
    running_max, normalizer, weighted = carried
    scale = queries.shape[-1] ** (-0.5)
    scores = (
        jnp.einsum("tkgd,nkd->tkgn", queries, key_rows, preferred_element_type=jnp.float32) * scale
    )
    visible = allowed[:, None, None, :]
    scores = jnp.where(visible, scores, LOWEST)
    new_max = jnp.maximum(running_max, jnp.max(scores, axis=-1))
    weights = jnp.where(visible, jnp.exp(scores - new_max[..., None]), 0.0)
    factor = jnp.exp(running_max - new_max)
    normalizer = normalizer * factor + jnp.sum(weights, axis=-1)
    weighted = weighted * factor[..., None] + jnp.einsum(
        "tkgn,nkd->tkgd",
        weights.astype(jnp.bfloat16),
        value_rows,
        preferred_element_type=jnp.float32,
    )
    return (new_max, normalizer, weighted)


def guarded_step(carried, queries, key_rows, value_rows, allowed):
    return lax.cond(
        jnp.any(allowed),
        lambda inner: online_step(inner, queries, key_rows, value_rows, allowed),
        lambda inner: inner,
        carried,
    )


def fold_rows(carried, queries, key_rows, value_rows, allowed):
    length = key_rows.shape[0]
    blocks = block_split(length)
    if blocks == 1:
        return guarded_step(carried, queries, key_rows, value_rows, allowed)
    width = length // blocks
    stacked = (
        key_rows.reshape((blocks, width) + key_rows.shape[1:]),
        value_rows.reshape((blocks, width) + value_rows.shape[1:]),
        allowed.reshape(allowed.shape[0], blocks, width).transpose(1, 0, 2),
    )

    def visit(inner_carry, parts):
        return (guarded_step(inner_carry, queries, parts[0], parts[1], parts[2]), None)

    carried, _ = lax.scan(visit, carried, stacked)
    return carried


def on_large(
    span_queries,
    span_keys,
    span_values,
    prefix_keys,
    prefix_values,
    prefix_lengths,
    decode_queries,
    decode_new_keys,
    decode_new_values,
    decode_key_cache,
    decode_value_cache,
    owner_map,
    decode_lengths,
):
    device = lax.axis_index("seq")
    tokens_here, heads_here, head_dim = span_queries.shape
    kv_here = span_keys.shape[1]
    group_size = heads_here // kv_here
    queries = span_queries.reshape(tokens_here, kv_here, group_size, head_dim)
    token_index = device * tokens_here + jnp.arange(tokens_here, dtype=jnp.int32)
    prefix_here = prefix_keys.shape[0]
    initial = (
        jnp.full((tokens_here, kv_here, group_size), LOWEST, jnp.float32),
        jnp.zeros((tokens_here, kv_here, group_size), jnp.float32),
        jnp.zeros((tokens_here, kv_here, group_size, head_dim), jnp.float32),
    )
    stride = prefix_here + tokens_here
    both_keys = jnp.concatenate([prefix_keys, span_keys], axis=0)
    both_values = jnp.concatenate([prefix_values, span_values], axis=0)
    carried = initial
    key_rows = lax.all_gather(both_keys, "seq", axis=0, tiled=True)
    value_rows = lax.all_gather(both_values, "seq", axis=0, tiled=True)
    length = key_rows.shape[0]
    shards = length // stride
    tail = key_rows.shape[1:]
    keys_split = key_rows.reshape((shards, stride) + tail)
    values_split = value_rows.reshape((shards, stride) + tail)
    prefix_k = keys_split[:, :prefix_here].reshape((shards * prefix_here,) + tail)
    prefix_v = values_split[:, :prefix_here].reshape((shards * prefix_here,) + tail)
    span_k = keys_split[:, prefix_here:].reshape((shards * tokens_here,) + tail)
    span_v = values_split[:, prefix_here:].reshape((shards * tokens_here,) + tail)
    prefix_position = jnp.arange(shards * prefix_here, dtype=jnp.int32)
    prefix_ok = prefix_position % prefix_here < lookup_small(
        prefix_lengths, prefix_position // prefix_here
    )
    carried = fold_rows(
        carried,
        queries,
        prefix_k,
        prefix_v,
        jnp.broadcast_to(prefix_ok[None, :], (tokens_here, prefix_k.shape[0])),
    )
    span_position = jnp.arange(shards * tokens_here, dtype=jnp.int32)
    carried = fold_rows(
        carried, queries, span_k, span_v, span_position[None, :] <= token_index[:, None]
    )
    _, normalizer, weighted = carried
    prefill_out = (
        (weighted / normalizer[..., None])
        .reshape(tokens_here, heads_here, head_dim)
        .astype(jnp.bfloat16)
    )
    owners = owner_map[:, 0]
    requests = owners.shape[0]
    order = jnp.arange(requests, dtype=jnp.int32)
    earlier = (owners[None, :] == owners[:, None]) & (order[None, :] < order[:, None])
    ranking = jnp.sum(earlier.astype(jnp.int32), axis=1)
    slots_here = decode_key_cache.shape[0]
    slot_ids = jnp.arange(slots_here, dtype=jnp.int32)
    query_rows = lax.all_gather(decode_queries, "seq", axis=0, tiled=True)
    new_keys = lax.all_gather(decode_new_keys, "seq", axis=0, tiled=True)
    new_values = lax.all_gather(decode_new_values, "seq", axis=0, tiled=True)
    chosen = (owners == device)[None, :] & (ranking[None, :] == slot_ids[:, None])
    selector = chosen.astype(jnp.bfloat16)
    picked_queries = jnp.einsum(
        "sn,nhd->shd", selector, query_rows, preferred_element_type=jnp.float32
    )
    picked_keys = jnp.einsum("sn,nkd->skd", selector, new_keys, preferred_element_type=jnp.float32)
    picked_values = jnp.einsum(
        "sn,nkd->skd", selector, new_values, preferred_element_type=jnp.float32
    )
    picked_lengths = jnp.sum(jnp.where(chosen, decode_lengths[None, :], 0), axis=1)
    context = decode_key_cache.shape[1]
    grouped = picked_queries.astype(jnp.bfloat16).reshape(slots_here, kv_here, group_size, head_dim)
    own_keys = picked_keys.astype(jnp.bfloat16)
    own_values = picked_values.astype(jnp.bfloat16)
    scale = head_dim ** (-0.5)
    scores = (
        jnp.einsum("skgd,sckd->skgc", grouped, decode_key_cache, preferred_element_type=jnp.float32)
        * scale
    )
    visible = (jnp.arange(context, dtype=jnp.int32)[None, :] < picked_lengths[:, None])[
        :, None, None, :
    ]
    scores = jnp.where(visible, scores, LOWEST)
    own_score = (
        jnp.einsum("skgd,skd->skg", grouped, own_keys, preferred_element_type=jnp.float32) * scale
    )
    top_score = jnp.maximum(jnp.max(scores, axis=-1), own_score)
    weights = jnp.where(visible, jnp.exp(scores - top_score[..., None]), 0.0)
    own_weight = jnp.exp(own_score - top_score)
    total_weight = jnp.sum(weights, axis=-1) + own_weight
    rounded_own = lax.optimization_barrier(own_weight.astype(jnp.bfloat16)).astype(jnp.float32)
    mixed = jnp.einsum(
        "skgc,sckd->skgd",
        weights.astype(jnp.bfloat16),
        decode_value_cache,
        preferred_element_type=jnp.float32,
    )
    mixed = mixed + rounded_own[..., None] * own_values.astype(jnp.float32)[:, :, None, :]
    count_here = jnp.sum((owners == device).astype(jnp.int32))
    used = (slot_ids < count_here)[:, None, None, None]
    decode_out = (
        jnp.where(used, mixed / total_weight[..., None], 0.0)
        .reshape(slots_here, heads_here, head_dim)
        .astype(jnp.bfloat16)
    )
    return (prefill_out, decode_out)


class Sizes:
    def __init__(self, group, span_queries, span_keys, prefix_keys, decode_queries, cache):
        self.n = group
        self.half = group // 2
        self.tokens, self.heads, self.dim = span_queries.shape
        self.kv = span_keys.shape[1]
        self.share = self.heads // self.kv
        self.rows = self.tokens * self.heads
        self.pre = prefix_keys.shape[0]
        self.pre_rows = self.pre * self.kv
        self.block = self.pre_rows + self.tokens * self.kv
        self.cols = self.half * self.block
        self.asks = decode_queries.shape[0]
        self.ask_at = 2 * self.block
        self.new_at = self.ask_at + self.asks * self.heads
        self.new_rows = 2 * self.asks * self.kv
        self.pack = self.new_at + self.new_rows
        self.slots, self.context = cache.shape[:2]
        self.cache_rows = self.context * self.kv
        self.stat_rows = PIECES * self.rows // self.dim
        self.pick_at = self.rows + self.stat_rows
        self.pick_new_at = self.slots * self.heads
        self.picks = self.pick_new_at + self.slots * self.new_rows
        self.back = self.pick_at + self.picks
        self.factor = self.dim**-0.5 * math.log2(math.e)

    def fits(self):
        power = self.n & (self.n - 1) == 0 and self.kv & (self.kv - 1) == 0
        return (
            power
            and 4 <= self.n <= 8
            and self.dim == 128
            and self.rows % 128 == 0
            and self.share % 16 == 0
            and self.block % 16 == 0
            and self.cols % 128 == 0
            and self.cache_rows % 128 == 0
            and self.new_rows == 8
        )


def column_tokens(z, me, table):
    lengths = [table[3 * z.slots + (me ^ j)] for j in range(z.half)]
    column = lax.broadcasted_iota(jnp.int32, (8, z.cols), 1)
    block = jnp.zeros((8, z.cols), jnp.int32)
    for j in range(1, z.half):
        block = block + (column >= z.block * j).astype(jnp.int32)
    within = column - block * z.block
    live = jnp.full((8, z.cols), lengths[0], jnp.int32)
    first = jnp.full((8, z.cols), me * z.tokens, jnp.int32)
    for j in range(1, z.half):
        live = jnp.where(block == j, lengths[j], live)
        first = jnp.where(block == j, (me ^ j) * z.tokens, first)
    place = within >> (z.kv.bit_length() - 1)
    token = jnp.where(
        within < z.pre_rows,
        jnp.where(place < live, -1, FAR_AWAY),
        first + place - z.pre,
    )
    head = within & (z.kv - 1)
    return [jnp.where(head == h, token, FAR_AWAY) for h in range(z.kv)]


def partial_attention(z, me, whose, query, near, table, score_ref, weight_ref, top_ref, sum_ref):
    keys = jnp.concatenate([b[0 : z.block, :] for b in near], axis=0)
    score_ref[...] = lax.dot_general(
        query[...], keys, (((1,), (1,)), ((), ())), preferred_element_type=jnp.float32
    )
    tokens = column_tokens(z, me, table)
    for t in range(z.tokens):
        for h in range(z.kv):
            at = t * z.heads + h * z.share
            seen = tokens[h] <= whose * z.tokens + t
            scores = score_ref[at : at + z.share, :].reshape(z.share // 8, 8, z.cols)
            scores = jnp.where(seen[None], scores, LOWEST)
            top = jnp.max(scores, axis=-1, keepdims=True)
            weights = jnp.exp2((scores - top) * z.factor)
            total = jnp.sum(weights, axis=-1, keepdims=True)
            flat = (z.share, z.dim)
            wide = (z.share // 8, 8, z.dim)
            top_ref[at : at + z.share, :] = jnp.broadcast_to(top, wide).reshape(flat)
            sum_ref[at : at + z.share, :] = jnp.broadcast_to(total, wide).reshape(flat)
            weight_ref[at : at + z.share, :] = weights.reshape(z.share, z.cols).astype(jnp.bfloat16)
    values = jnp.concatenate([b[z.block : 2 * z.block, :] for b in near], axis=0)
    return jnp.dot(weight_ref[...], values, preferred_element_type=jnp.float32)


def plan_kernel(z):
    def body(owners, lengths, cached, table):
        me = lax.axis_index("seq")
        partner = me ^ z.half
        for i in range(2 * z.slots):
            table[i] = -1

        def visit(r, counts):
            mine = owners[r] == me
            theirs = owners[r] == partner

            @pl.when(mine)
            def _():
                table[counts[0]] = r
                table[2 * z.slots + counts[0]] = cached[r]

            @pl.when(theirs)
            def _():
                table[z.slots + counts[1]] = r

            return (counts[0] + mine.astype(jnp.int32), counts[1] + theirs.astype(jnp.int32))

        lax.fori_loop(0, z.n * z.asks, visit, (jnp.int32(0), jnp.int32(0)))
        for i in range(z.n):
            table[3 * z.slots + i] = lengths[i]

    return body


def pick_near(z, me, near, request):
    ask = jnp.zeros((z.heads, z.dim), jnp.bfloat16)
    new = jnp.zeros((z.new_rows, z.dim), jnp.bfloat16)
    for j in range(z.half):
        for a in range(z.asks):
            hit = request == (me ^ j) * z.asks + a
            at = z.ask_at + a * z.heads
            ask = jnp.where(hit, near[j][at : at + z.heads, :], ask)
            if a == 0:
                new = jnp.where(
                    (request >= 0) & (lax.div(request, z.asks) == (me ^ j)),
                    near[j][z.new_at : z.pack, :],
                    new,
                )
    return ask, new


def pieces_of(x):
    first = x.astype(jnp.bfloat16).astype(jnp.float32)
    second = (x - first).astype(jnp.bfloat16).astype(jnp.float32)
    third = (x - first - second).astype(jnp.bfloat16).astype(jnp.float32)
    return [first, second, third]


def pack_kernel(z):
    def body(*refs):
        out, new, sems = refs[-3:]
        copies, at = [], 0
        for i, ref in enumerate(refs[:7]):
            rows = ref.shape[0]
            into = out.at[pl.ds(at, rows), :] if i < 5 else new.at[i - 5]
            copies.append(pltpu.make_async_copy(ref, into, sems.at[i]))
            at += rows
        for copy in reversed(copies):
            copy.start()
        for copy in reversed(copies):
            copy.wait()
        both = [new[i].astype(jnp.float32) for i in range(2)]
        out[z.new_at : z.pack, :] = jnp.concatenate(both, axis=0).astype(jnp.bfloat16)

    return body


def turn_stats(z, top_ref, sum_ref):
    lane = lax.broadcasted_iota(jnp.int32, (z.rows, z.dim), 1)
    return jnp.transpose(jnp.where(lane == 0, top_ref[...], sum_ref[...]))[:8, :]


def pick_all(z, me, table, first, near, out):
    for s in range(z.slots):
        ask, new = pick_near(z, me, near, table[first + s])
        out[s * z.heads : (s + 1) * z.heads, :] = ask
        at = z.pick_new_at + s * z.new_rows
        out[at : at + z.new_rows, :] = new


def select_kernel(z):
    def body(table, *refs):
        pick_all(z, lax.axis_index("seq"), table, z.slots, refs[:-1], refs[-1])

    return body


def far_kernel(z):
    def body(table, query, asked, *refs):
        near, back, scratch = refs[: z.half], refs[z.half], refs[z.half + 1 :]
        score_ref, weight_ref, top_ref, sum_ref = scratch
        me = lax.axis_index("seq")
        back[z.pick_at : z.back, :] = asked[...]
        mixed = partial_attention(
            z, me, me ^ z.half, query, near, table, score_ref, weight_ref, top_ref, sum_ref
        )
        total = sum_ref[...]
        back[0 : z.rows, :] = (mixed / total).astype(jnp.bfloat16)
        stats = turn_stats(z, top_ref, sum_ref)
        pieces = pieces_of(stats[0:1, :]) + pieces_of(stats[1:2, :])
        row = lax.broadcasted_iota(jnp.int32, (PIECES, z.rows), 0)
        turned = jnp.zeros((PIECES, z.rows), jnp.float32)
        for i, piece in enumerate(pieces):
            turned = jnp.where(row == i, piece, turned)
        for i in range(z.rows // z.dim):
            back[z.rows + PIECES * i : z.rows + PIECES * (i + 1), :] = turned[
                :, i * z.dim : (i + 1) * z.dim
            ].astype(jnp.bfloat16)

    return body


def own_kernel(z):
    def body(table, query, *refs):
        near, (mixed, stats, mine) = refs[: z.half], refs[z.half : z.half + 3]
        score_ref, weight_ref, top_ref, sum_ref = refs[z.half + 3 :]
        me = lax.axis_index("seq")
        pick_all(z, me, table, 0, near, mine)
        mixed[...] = partial_attention(
            z, me, me, query, near, table, score_ref, weight_ref, top_ref, sum_ref
        )
        stats[...] = turn_stats(z, top_ref, sum_ref)

    return body


def last_kernel(z):
    def body(table, mixed, stats, mine, back, keys, values, *outs):
        out_hbm, decoded_hbm, out, decoded, sems = outs
        pieces = jnp.concatenate(
            [
                back[z.rows + PIECES * i : z.rows + PIECES * (i + 1), :].astype(jnp.float32)
                for i in range(z.rows // z.dim)
            ],
            axis=1,
        )
        far_top = pieces[0:1, :] + pieces[1:2, :] + pieces[2:3, :]
        far_sum = pieces[3:4, :] + pieces[4:5, :] + pieces[5:6, :]
        own_top, own_sum = stats[0:1, :], stats[1:2, :]
        top = jnp.maximum(own_top, far_top)
        here = jnp.exp2((own_top - top) * z.factor)
        there = jnp.exp2((far_top - top) * z.factor) * far_sum
        inverse = 1.0 / (own_sum * here + there)
        row = lax.broadcasted_iota(jnp.int32, (z.dim, z.rows), 0)
        shares = jnp.transpose(jnp.where(row == 0, here * inverse, there * inverse))
        joined = (
            mixed[...] * shares[:, 0:1] + back[0 : z.rows, :].astype(jnp.float32) * shares[:, 1:2]
        )
        out[...] = joined.astype(jnp.bfloat16)
        first_copy = pltpu.make_async_copy(out, out_hbm, sems.at[0])
        first_copy.start()
        decode(z, table, mine, back, keys, values, decoded)
        second_copy = pltpu.make_async_copy(decoded, decoded_hbm, sems.at[1])
        second_copy.start()
        first_copy.wait()
        second_copy.wait()

    return body


def decode(z, table, mine, back, keys, values, decoded):
    me = lax.axis_index("seq")
    column = lax.broadcasted_iota(jnp.int32, (z.heads, z.cache_rows), 1)
    row = lax.broadcasted_iota(jnp.int32, (z.heads, z.cache_rows), 0)
    shift = z.share.bit_length() - 1
    match = (column & (z.kv - 1)) == (row >> shift)
    place = column >> (z.kv.bit_length() - 1)
    head_of = lax.broadcasted_iota(jnp.int32, (z.heads, z.dim), 0) >> shift
    asks, news, scores = [], [], []
    for s in range(z.slots):
        source = lax.div(jnp.maximum(table[s], 0), z.asks)
        from_far = (source ^ me) >= z.half
        here = s * z.heads
        there = z.pick_at + here
        ask = back[there : there + z.heads, :]
        asks.append(jnp.where(from_far, ask, mine[here : here + z.heads, :]))
        here = z.pick_new_at + s * z.new_rows
        there = z.pick_at + here
        new = back[there : there + z.new_rows, :]
        new = jnp.where(from_far, new, mine[here : here + z.new_rows, :])
        news.append(new.astype(jnp.float32))
    for s in range(z.slots):
        scores.append(
            lax.dot_general(
                asks[s],
                keys[s * z.cache_rows : (s + 1) * z.cache_rows, :],
                (((1,), (1,)), ((), ())),
                preferred_element_type=jnp.float32,
            )
        )
    weights, rests = [], []
    for s in range(z.slots):
        safe = jnp.maximum(table[s], 0)
        at = safe - lax.div(safe, z.asks) * z.asks
        new = news[s]
        new_key = jnp.zeros((z.heads, z.dim), jnp.float32)
        new_value = jnp.zeros((z.heads, z.dim), jnp.float32)
        for a in range(z.asks):
            for h in range(z.kv):
                here_now = (head_of == h) & (at == a)
                i = a * z.kv + h
                new_key = jnp.where(here_now, new[i : i + 1, :], new_key)
                i = i + z.asks * z.kv
                new_value = jnp.where(here_now, new[i : i + 1, :], new_value)
        own = jnp.sum(asks[s].astype(jnp.float32) * new_key, axis=-1, keepdims=True)
        seen = jnp.where(match & (place < table[2 * z.slots + s]), scores[s], LOWEST)
        peak = jnp.maximum(jnp.max(seen, axis=-1, keepdims=True), own)
        weight = jnp.exp2((seen - peak) * z.factor)
        own_weight = jnp.exp2((own - peak) * z.factor)
        total = jnp.sum(weight, axis=-1, keepdims=True) + own_weight
        weights.append(weight.astype(jnp.bfloat16))
        rests.append((own_weight.astype(jnp.bfloat16).astype(jnp.float32) * new_value, total))
    for s in range(z.slots):
        result = jnp.dot(
            weights[s],
            values[s * z.cache_rows : (s + 1) * z.cache_rows, :],
            preferred_element_type=jnp.float32,
        )
        result = (result + rests[s][0]) / rests[s][1]
        decoded[s * z.heads : (s + 1) * z.heads, :] = jnp.where(
            table[s] >= 0, result, 0.0
        ).astype(jnp.bfloat16)


def swap(x, n, by):
    return lax.ppermute(x, "seq", [(i, i ^ by) for i in range(n)])


def on_small(
    z,
    span_queries,
    span_keys,
    span_values,
    prefix_keys,
    prefix_values,
    prefix_lengths,
    decode_queries,
    decode_new_keys,
    decode_new_values,
    decode_key_cache,
    decode_value_cache,
    owner_map,
    decode_lengths,
):
    def flat(x):
        return x.reshape(-1, z.dim)

    def local(x):
        return pltpu.with_memory_space_constraint(x, pltpu.VMEM)

    smem = pl.BlockSpec(memory_space=pltpu.SMEM)
    vmem = pl.BlockSpec(memory_space=pltpu.VMEM)
    hbm = pl.BlockSpec(memory_space=pl.ANY)

    def ints(x):
        return pltpu.with_memory_space_constraint(x, pltpu.SMEM)

    queries = flat(span_queries)
    far_queries = local(swap(queries, z.n, z.half))
    packed = pl.pallas_call(
        pack_kernel(z),
        out_shape=pltpu.VMEM((z.pack, z.dim), jnp.bfloat16),
        in_specs=[hbm] * 7,
        out_specs=vmem,
        scratch_shapes=[
            pltpu.VMEM((2, z.asks * z.kv, z.dim), jnp.bfloat16),
            pltpu.SemaphoreType.DMA((7,)),
        ],
        name="pack",
    )(
        flat(prefix_keys),
        flat(span_keys),
        flat(prefix_values),
        flat(span_values),
        flat(decode_queries),
        flat(decode_new_keys),
        flat(decode_new_values),
    )
    near = [local(packed)]
    for j in range(1, z.half):
        near.append(local(swap(packed, z.n, j)))
    table = pl.pallas_call(
        plan_kernel(z),
        out_shape=pltpu.SMEM((3 * z.slots + z.n,), jnp.int32),
        in_specs=[smem] * 3,
        out_specs=smem,
        name="plan",
    )(owner_map.reshape(-1), prefix_lengths, decode_lengths)
    table = ints(table)
    asked = pl.pallas_call(
        select_kernel(z),
        out_shape=pltpu.VMEM((z.picks, z.dim), jnp.bfloat16),
        in_specs=[smem] + [vmem] * z.half,
        out_specs=vmem,
        name="select",
    )(table, *near)
    wide = [pltpu.VMEM((z.rows, z.cols), jnp.float32), pltpu.VMEM((z.rows, z.cols), jnp.bfloat16)]
    wide += [pltpu.VMEM((z.rows, z.dim), jnp.float32)] * 2
    sent = pl.pallas_call(
        far_kernel(z),
        out_shape=pltpu.VMEM((z.back, z.dim), jnp.bfloat16),
        in_specs=[smem] + [vmem] * (2 + z.half),
        out_specs=vmem,
        scratch_shapes=wide,
        name="far_part",
    )(table, far_queries, local(asked), *near)
    back = local(swap(sent, z.n, z.half))
    held = pl.pallas_call(
        own_kernel(z),
        out_shape=[
            pltpu.VMEM((z.rows, z.dim), jnp.float32),
            pltpu.VMEM((8, z.rows), jnp.float32),
            pltpu.VMEM((z.picks, z.dim), jnp.bfloat16),
        ],
        in_specs=[smem] + [vmem] * (1 + z.half),
        out_specs=[vmem] * 3,
        scratch_shapes=wide,
        name="own_part",
    )(table, local(queries), *near)
    out, decoded = pl.pallas_call(
        last_kernel(z),
        out_shape=[
            jax.ShapeDtypeStruct((z.rows, z.dim), jnp.bfloat16),
            jax.ShapeDtypeStruct((z.slots * z.heads, z.dim), jnp.bfloat16),
        ],
        in_specs=[smem] + [vmem] * 6,
        out_specs=[hbm, hbm],
        scratch_shapes=[
            pltpu.VMEM((z.rows, z.dim), jnp.bfloat16),
            pltpu.VMEM((z.slots * z.heads, z.dim), jnp.bfloat16),
            pltpu.SemaphoreType.DMA((2,)),
        ],
        name="last_part",
    )(
        table,
        *[local(x) for x in held],
        back,
        local(flat(decode_key_cache)),
        local(flat(decode_value_cache)),
    )
    return (
        out.reshape(z.tokens, z.heads, z.dim),
        decoded.reshape(z.slots, z.heads, z.dim),
    )


def solution(mesh):
    group = mesh.shape["seq"]

    def on_device(*args):
        z = Sizes(group, args[0], args[1], args[3], args[6], args[9])
        if z.fits():
            return on_small(z, *args)
        return on_large(*args)

    return jax.shard_map(
        on_device,
        mesh=mesh,
        in_specs=(
            P(("groups", "seq"), "tp", None),
            P(("groups", "seq"), "tp", None),
            P(("groups", "seq"), "tp", None),
            P(("groups", "seq"), "tp", None),
            P(("groups", "seq"), "tp", None),
            P("groups"),
            P(("groups", "seq"), "tp", None),
            P(("groups", "seq"), "tp", None),
            P(("groups", "seq"), "tp", None),
            P(("groups", "seq"), None, "tp", None),
            P(("groups", "seq"), None, "tp", None),
            P("groups", None),
            P("groups"),
        ),
        out_specs=(P(("groups", "seq"), "tp", None), P(("groups", "seq"), "tp", None)),
        check_vma=False,
    )
```

```python
import math

import jax
import jax.numpy as jnp
from jax import lax
from jax.experimental import pallas as pl
from jax.experimental.pallas import tpu as pltpu
from jax.sharding import PartitionSpec as P


LOWEST = -1e30
FAR_AWAY = 1 << 30
PIECES = 8


def lookup_small(table, wanted):
    columns = jnp.arange(table.shape[0], dtype=jnp.int32)
    return jnp.sum(jnp.where(wanted[:, None] == columns[None, :], table[None, :], 0), axis=1)


def block_split(length):
    blocks = 1
    while length // blocks > 512 or length % blocks != 0:
        blocks += 1
    return blocks


def online_step(carried, queries, key_rows, value_rows, allowed):
    running_max, normalizer, weighted = carried
    scale = queries.shape[-1] ** (-0.5)
    scores = (
        jnp.einsum("tkgd,nkd->tkgn", queries, key_rows, preferred_element_type=jnp.float32) * scale
    )
    visible = allowed[:, None, None, :]
    scores = jnp.where(visible, scores, LOWEST)
    new_max = jnp.maximum(running_max, jnp.max(scores, axis=-1))
    weights = jnp.where(visible, jnp.exp(scores - new_max[..., None]), 0.0)
    factor = jnp.exp(running_max - new_max)
    normalizer = normalizer * factor + jnp.sum(weights, axis=-1)
    weighted = weighted * factor[..., None] + jnp.einsum(
        "tkgn,nkd->tkgd",
        weights.astype(jnp.bfloat16),
        value_rows,
        preferred_element_type=jnp.float32,
    )
    return (new_max, normalizer, weighted)


def guarded_step(carried, queries, key_rows, value_rows, allowed):
    return lax.cond(
        jnp.any(allowed),
        lambda inner: online_step(inner, queries, key_rows, value_rows, allowed),
        lambda inner: inner,
        carried,
    )


def fold_rows(carried, queries, key_rows, value_rows, allowed):
    length = key_rows.shape[0]
    blocks = block_split(length)
    if blocks == 1:
        return guarded_step(carried, queries, key_rows, value_rows, allowed)
    width = length // blocks
    stacked = (
        key_rows.reshape((blocks, width) + key_rows.shape[1:]),
        value_rows.reshape((blocks, width) + value_rows.shape[1:]),
        allowed.reshape(allowed.shape[0], blocks, width).transpose(1, 0, 2),
    )

    def visit(inner_carry, parts):
        return (guarded_step(inner_carry, queries, parts[0], parts[1], parts[2]), None)

    carried, _ = lax.scan(visit, carried, stacked)
    return carried


def on_large(
    span_queries,
    span_keys,
    span_values,
    prefix_keys,
    prefix_values,
    prefix_lengths,
    decode_queries,
    decode_new_keys,
    decode_new_values,
    decode_key_cache,
    decode_value_cache,
    owner_map,
    decode_lengths,
):
    device = lax.axis_index("seq")
    tokens_here, heads_here, head_dim = span_queries.shape
    kv_here = span_keys.shape[1]
    group_size = heads_here // kv_here
    queries = span_queries.reshape(tokens_here, kv_here, group_size, head_dim)
    token_index = device * tokens_here + jnp.arange(tokens_here, dtype=jnp.int32)
    prefix_here = prefix_keys.shape[0]
    initial = (
        jnp.full((tokens_here, kv_here, group_size), LOWEST, jnp.float32),
        jnp.zeros((tokens_here, kv_here, group_size), jnp.float32),
        jnp.zeros((tokens_here, kv_here, group_size, head_dim), jnp.float32),
    )
    stride = prefix_here + tokens_here
    both_keys = jnp.concatenate([prefix_keys, span_keys], axis=0)
    both_values = jnp.concatenate([prefix_values, span_values], axis=0)
    carried = initial
    key_rows = lax.all_gather(both_keys, "seq", axis=0, tiled=True)
    value_rows = lax.all_gather(both_values, "seq", axis=0, tiled=True)
    length = key_rows.shape[0]
    shards = length // stride
    tail = key_rows.shape[1:]
    keys_split = key_rows.reshape((shards, stride) + tail)
    values_split = value_rows.reshape((shards, stride) + tail)
    prefix_k = keys_split[:, :prefix_here].reshape((shards * prefix_here,) + tail)
    prefix_v = values_split[:, :prefix_here].reshape((shards * prefix_here,) + tail)
    span_k = keys_split[:, prefix_here:].reshape((shards * tokens_here,) + tail)
    span_v = values_split[:, prefix_here:].reshape((shards * tokens_here,) + tail)
    prefix_position = jnp.arange(shards * prefix_here, dtype=jnp.int32)
    prefix_ok = prefix_position % prefix_here < lookup_small(
        prefix_lengths, prefix_position // prefix_here
    )
    carried = fold_rows(
        carried,
        queries,
        prefix_k,
        prefix_v,
        jnp.broadcast_to(prefix_ok[None, :], (tokens_here, prefix_k.shape[0])),
    )
    span_position = jnp.arange(shards * tokens_here, dtype=jnp.int32)
    carried = fold_rows(
        carried, queries, span_k, span_v, span_position[None, :] <= token_index[:, None]
    )
    _, normalizer, weighted = carried
    prefill_out = (
        (weighted / normalizer[..., None])
        .reshape(tokens_here, heads_here, head_dim)
        .astype(jnp.bfloat16)
    )
    owners = owner_map[:, 0]
    requests = owners.shape[0]
    order = jnp.arange(requests, dtype=jnp.int32)
    earlier = (owners[None, :] == owners[:, None]) & (order[None, :] < order[:, None])
    ranking = jnp.sum(earlier.astype(jnp.int32), axis=1)
    slots_here = decode_key_cache.shape[0]
    slot_ids = jnp.arange(slots_here, dtype=jnp.int32)
    query_rows = lax.all_gather(decode_queries, "seq", axis=0, tiled=True)
    new_keys = lax.all_gather(decode_new_keys, "seq", axis=0, tiled=True)
    new_values = lax.all_gather(decode_new_values, "seq", axis=0, tiled=True)
    chosen = (owners == device)[None, :] & (ranking[None, :] == slot_ids[:, None])
    selector = chosen.astype(jnp.bfloat16)
    picked_queries = jnp.einsum(
        "sn,nhd->shd", selector, query_rows, preferred_element_type=jnp.float32
    )
    picked_keys = jnp.einsum("sn,nkd->skd", selector, new_keys, preferred_element_type=jnp.float32)
    picked_values = jnp.einsum(
        "sn,nkd->skd", selector, new_values, preferred_element_type=jnp.float32
    )
    picked_lengths = jnp.sum(jnp.where(chosen, decode_lengths[None, :], 0), axis=1)
    context = decode_key_cache.shape[1]
    grouped = picked_queries.astype(jnp.bfloat16).reshape(slots_here, kv_here, group_size, head_dim)
    own_keys = picked_keys.astype(jnp.bfloat16)
    own_values = picked_values.astype(jnp.bfloat16)
    scale = head_dim ** (-0.5)
    scores = (
        jnp.einsum("skgd,sckd->skgc", grouped, decode_key_cache, preferred_element_type=jnp.float32)
        * scale
    )
    visible = (jnp.arange(context, dtype=jnp.int32)[None, :] < picked_lengths[:, None])[
        :, None, None, :
    ]
    scores = jnp.where(visible, scores, LOWEST)
    own_score = (
        jnp.einsum("skgd,skd->skg", grouped, own_keys, preferred_element_type=jnp.float32) * scale
    )
    top_score = jnp.maximum(jnp.max(scores, axis=-1), own_score)
    weights = jnp.where(visible, jnp.exp(scores - top_score[..., None]), 0.0)
    own_weight = jnp.exp(own_score - top_score)
    total_weight = jnp.sum(weights, axis=-1) + own_weight
    rounded_own = lax.optimization_barrier(own_weight.astype(jnp.bfloat16)).astype(jnp.float32)
    mixed = jnp.einsum(
        "skgc,sckd->skgd",
        weights.astype(jnp.bfloat16),
        decode_value_cache,
        preferred_element_type=jnp.float32,
    )
    mixed = mixed + rounded_own[..., None] * own_values.astype(jnp.float32)[:, :, None, :]
    count_here = jnp.sum((owners == device).astype(jnp.int32))
    used = (slot_ids < count_here)[:, None, None, None]
    decode_out = (
        jnp.where(used, mixed / total_weight[..., None], 0.0)
        .reshape(slots_here, heads_here, head_dim)
        .astype(jnp.bfloat16)
    )
    return (prefill_out, decode_out)


class Sizes:
    def __init__(self, group, span_queries, span_keys, prefix_keys, decode_queries, cache):
        self.n = group
        self.half = group // 2
        self.far = self.half
        self.offsets = [j for j in range(group) if not j & self.far]
        self.tokens, self.heads, self.dim = span_queries.shape
        self.kv = span_keys.shape[1]
        self.share = self.heads // self.kv
        self.rows = self.tokens * self.heads
        self.pre = prefix_keys.shape[0]
        self.pre_rows = self.pre * self.kv
        self.block = self.pre_rows + self.tokens * self.kv
        self.cols = self.half * self.block
        self.asks = decode_queries.shape[0]
        self.ask_at = 2 * self.block
        self.new_at = self.ask_at + self.asks * self.heads
        self.new_rows = 2 * self.asks * self.kv
        self.pack = self.new_at + self.new_rows
        self.slots, self.context = cache.shape[:2]
        self.cache_rows = self.context * self.kv
        self.stat_rows = PIECES * self.rows // self.dim
        self.pick_at = self.rows + self.stat_rows
        self.pick_new_at = self.slots * self.heads
        self.picks = self.pick_new_at + self.slots * self.new_rows
        self.back = self.pick_at + self.picks
        self.factor = self.dim**-0.5 * math.log2(math.e)

    def fits(self):
        power = self.n & (self.n - 1) == 0 and self.kv & (self.kv - 1) == 0
        return (
            power
            and 4 <= self.n <= 8
            and self.dim == 128
            and self.rows % 128 == 0
            and self.share % 16 == 0
            and self.block % 16 == 0
            and self.cols % 128 == 0
            and self.cache_rows % 128 == 0
            and self.new_rows == 8
        )


def column_tokens(z, me, table):
    lengths = [table[3 * z.slots + (me ^ j)] for j in z.offsets]
    column = lax.broadcasted_iota(jnp.int32, (8, z.cols), 1)
    block = jnp.zeros((8, z.cols), jnp.int32)
    for j in range(1, z.half):
        block = block + (column >= z.block * j).astype(jnp.int32)
    within = column - block * z.block
    live = jnp.full((8, z.cols), lengths[0], jnp.int32)
    first = jnp.full((8, z.cols), me * z.tokens, jnp.int32)
    for j in range(1, z.half):
        live = jnp.where(block == j, lengths[j], live)
        first = jnp.where(block == j, (me ^ z.offsets[j]) * z.tokens, first)
    place = within >> (z.kv.bit_length() - 1)
    token = jnp.where(
        within < z.pre_rows,
        jnp.where(place < live, -1, FAR_AWAY),
        first + place - z.pre,
    )
    head = within & (z.kv - 1)
    return [jnp.where(head == h, token, FAR_AWAY) for h in range(z.kv)]


def partial_attention(z, me, whose, query, near, table, score_ref, weight_ref, top_ref, sum_ref):
    keys = jnp.concatenate([b[0 : z.block, :] for b in near], axis=0)
    score_ref[...] = lax.dot_general(
        query[...], keys, (((1,), (1,)), ((), ())), preferred_element_type=jnp.float32
    )
    tokens = column_tokens(z, me, table)
    for t in range(z.tokens):
        for h in range(z.kv):
            at = t * z.heads + h * z.share
            seen = tokens[h] <= whose * z.tokens + t
            scores = score_ref[at : at + z.share, :].reshape(z.share // 8, 8, z.cols)
            scores = jnp.where(seen[None], scores, LOWEST)
            top = jnp.max(scores, axis=-1, keepdims=True)
            weights = jnp.exp2((scores - top) * z.factor)
            total = jnp.sum(weights, axis=-1, keepdims=True)
            flat = (z.share, z.dim)
            wide = (z.share // 8, 8, z.dim)
            top_ref[at : at + z.share, :] = jnp.broadcast_to(top, wide).reshape(flat)
            sum_ref[at : at + z.share, :] = jnp.broadcast_to(total, wide).reshape(flat)
            weight_ref[at : at + z.share, :] = weights.reshape(z.share, z.cols).astype(jnp.bfloat16)
    values = jnp.concatenate([b[z.block : 2 * z.block, :] for b in near], axis=0)
    return jnp.dot(weight_ref[...], values, preferred_element_type=jnp.float32)


def plan_kernel(z):
    def body(owners, lengths, cached, table):
        me = lax.axis_index("seq")
        partner = me ^ z.far
        for i in range(2 * z.slots):
            table[i] = -1

        def visit(r, counts):
            mine = owners[r] == me
            theirs = owners[r] == partner

            @pl.when(mine)
            def _():
                table[counts[0]] = r
                table[2 * z.slots + counts[0]] = cached[r]

            @pl.when(theirs)
            def _():
                table[z.slots + counts[1]] = r

            return (counts[0] + mine.astype(jnp.int32), counts[1] + theirs.astype(jnp.int32))

        lax.fori_loop(0, z.n * z.asks, visit, (jnp.int32(0), jnp.int32(0)))
        for i in range(z.n):
            table[3 * z.slots + i] = lengths[i]

    return body


def pick_near(z, me, near, request):
    ask = jnp.zeros((z.heads, z.dim), jnp.bfloat16)
    new = jnp.zeros((z.new_rows, z.dim), jnp.bfloat16)
    for j in range(z.half):
        for a in range(z.asks):
            hit = request == (me ^ z.offsets[j]) * z.asks + a
            at = z.ask_at + a * z.heads
            ask = jnp.where(hit, near[j][at : at + z.heads, :], ask)
            if a == 0:
                new = jnp.where(
                    (request >= 0) & (lax.div(request, z.asks) == (me ^ z.offsets[j])),
                    near[j][z.new_at : z.pack, :],
                    new,
                )
    return ask, new


def pieces_of(x):
    first = x.astype(jnp.bfloat16).astype(jnp.float32)
    second = (x - first).astype(jnp.bfloat16).astype(jnp.float32)
    third = (x - first - second).astype(jnp.bfloat16).astype(jnp.float32)
    return [first, second, third]


def pack_kernel(z):
    def body(*refs):
        out, new, sems = refs[-3:]
        copies, at = [], 0
        for i, ref in enumerate(refs[:7]):
            rows = ref.shape[0]
            into = out.at[pl.ds(at, rows), :] if i < 5 else new.at[i - 5]
            copies.append(pltpu.make_async_copy(ref, into, sems.at[i]))
            at += rows
        for copy in reversed(copies):
            copy.start()
        for copy in reversed(copies):
            copy.wait()
        both = [new[i].astype(jnp.float32) for i in range(2)]
        out[z.new_at : z.pack, :] = jnp.concatenate(both, axis=0).astype(jnp.bfloat16)

    return body


def turn_stats(z, top_ref, sum_ref):
    lane = lax.broadcasted_iota(jnp.int32, (z.rows, z.dim), 1)
    return jnp.transpose(jnp.where(lane == 0, top_ref[...], sum_ref[...]))[:8, :]


def pick_all(z, me, table, first, near, out):
    for s in range(z.slots):
        ask, new = pick_near(z, me, near, table[first + s])
        out[s * z.heads : (s + 1) * z.heads, :] = ask
        at = z.pick_new_at + s * z.new_rows
        out[at : at + z.new_rows, :] = new


def select_kernel(z):
    def body(table, *refs):
        pick_all(z, lax.axis_index("seq"), table, z.slots, refs[:-1], refs[-1])

    return body


def far_kernel(z):
    def body(table, query, asked, *refs):
        near, back, scratch = refs[: z.half], refs[z.half], refs[z.half + 1 :]
        score_ref, weight_ref, top_ref, sum_ref = scratch
        me = lax.axis_index("seq")
        back[z.pick_at : z.back, :] = asked[...]
        mixed = partial_attention(
            z, me, me ^ z.far, query, near, table, score_ref, weight_ref, top_ref, sum_ref
        )
        total = sum_ref[...]
        back[0 : z.rows, :] = (mixed / total).astype(jnp.bfloat16)
        stats = turn_stats(z, top_ref, sum_ref)
        pieces = pieces_of(stats[0:1, :]) + pieces_of(stats[1:2, :])
        row = lax.broadcasted_iota(jnp.int32, (PIECES, z.rows), 0)
        turned = jnp.zeros((PIECES, z.rows), jnp.float32)
        for i, piece in enumerate(pieces):
            turned = jnp.where(row == i, piece, turned)
        for i in range(z.rows // z.dim):
            back[z.rows + PIECES * i : z.rows + PIECES * (i + 1), :] = turned[
                :, i * z.dim : (i + 1) * z.dim
            ].astype(jnp.bfloat16)

    return body


def own_kernel(z):
    def body(table, query, *refs):
        near, (mixed, stats, mine) = refs[: z.half], refs[z.half : z.half + 3]
        score_ref, weight_ref, top_ref, sum_ref = refs[z.half + 3 :]
        me = lax.axis_index("seq")
        pick_all(z, me, table, 0, near, mine)
        mixed[...] = partial_attention(
            z, me, me, query, near, table, score_ref, weight_ref, top_ref, sum_ref
        )
        stats[...] = turn_stats(z, top_ref, sum_ref)

    return body


def last_kernel(z):
    def body(table, mixed, stats, mine, back, keys, values, *outs):
        out_hbm, decoded_hbm, out, decoded, sems = outs
        pieces = jnp.concatenate(
            [
                back[z.rows + PIECES * i : z.rows + PIECES * (i + 1), :].astype(jnp.float32)
                for i in range(z.rows // z.dim)
            ],
            axis=1,
        )
        far_top = pieces[0:1, :] + pieces[1:2, :] + pieces[2:3, :]
        far_sum = pieces[3:4, :] + pieces[4:5, :] + pieces[5:6, :]
        own_top, own_sum = stats[0:1, :], stats[1:2, :]
        top = jnp.maximum(own_top, far_top)
        here = jnp.exp2((own_top - top) * z.factor)
        there = jnp.exp2((far_top - top) * z.factor) * far_sum
        inverse = 1.0 / (own_sum * here + there)
        row = lax.broadcasted_iota(jnp.int32, (z.dim, z.rows), 0)
        shares = jnp.transpose(jnp.where(row == 0, here * inverse, there * inverse))
        joined = (
            mixed[...] * shares[:, 0:1] + back[0 : z.rows, :].astype(jnp.float32) * shares[:, 1:2]
        )
        out[...] = joined.astype(jnp.bfloat16)
        first_copy = pltpu.make_async_copy(out, out_hbm, sems.at[0])
        first_copy.start()
        decode(z, table, mine, back, keys, values, decoded)
        second_copy = pltpu.make_async_copy(decoded, decoded_hbm, sems.at[1])
        second_copy.start()
        first_copy.wait()
        second_copy.wait()

    return body


def decode(z, table, mine, back, keys, values, decoded):
    me = lax.axis_index("seq")
    column = lax.broadcasted_iota(jnp.int32, (z.heads, z.cache_rows), 1)
    row = lax.broadcasted_iota(jnp.int32, (z.heads, z.cache_rows), 0)
    shift = z.share.bit_length() - 1
    match = (column & (z.kv - 1)) == (row >> shift)
    place = column >> (z.kv.bit_length() - 1)
    head_of = lax.broadcasted_iota(jnp.int32, (z.heads, z.dim), 0) >> shift
    asks, news, scores = [], [], []
    for s in range(z.slots):
        source = lax.div(jnp.maximum(table[s], 0), z.asks)
        from_far = ((source ^ me) & z.far) != 0
        here = s * z.heads
        there = z.pick_at + here
        ask = back[there : there + z.heads, :]
        asks.append(jnp.where(from_far, ask, mine[here : here + z.heads, :]))
        here = z.pick_new_at + s * z.new_rows
        there = z.pick_at + here
        new = back[there : there + z.new_rows, :]
        new = jnp.where(from_far, new, mine[here : here + z.new_rows, :])
        news.append(new.astype(jnp.float32))
    for s in range(z.slots):
        scores.append(
            lax.dot_general(
                asks[s],
                keys[s * z.cache_rows : (s + 1) * z.cache_rows, :],
                (((1,), (1,)), ((), ())),
                preferred_element_type=jnp.float32,
            )
        )
    weights, rests = [], []
    for s in range(z.slots):
        safe = jnp.maximum(table[s], 0)
        at = safe - lax.div(safe, z.asks) * z.asks
        new = news[s]
        new_key = jnp.zeros((z.heads, z.dim), jnp.float32)
        new_value = jnp.zeros((z.heads, z.dim), jnp.float32)
        for a in range(z.asks):
            for h in range(z.kv):
                here_now = (head_of == h) & (at == a)
                i = a * z.kv + h
                new_key = jnp.where(here_now, new[i : i + 1, :], new_key)
                i = i + z.asks * z.kv
                new_value = jnp.where(here_now, new[i : i + 1, :], new_value)
        own = jnp.sum(asks[s].astype(jnp.float32) * new_key, axis=-1, keepdims=True)
        seen = jnp.where(match & (place < table[2 * z.slots + s]), scores[s], LOWEST)
        peak = jnp.maximum(jnp.max(seen, axis=-1, keepdims=True), own)
        weight = jnp.exp2((seen - peak) * z.factor)
        own_weight = jnp.exp2((own - peak) * z.factor)
        total = jnp.sum(weight, axis=-1, keepdims=True) + own_weight
        weights.append(weight.astype(jnp.bfloat16))
        rests.append((own_weight.astype(jnp.bfloat16).astype(jnp.float32) * new_value, total))
    for s in range(z.slots):
        result = jnp.dot(
            weights[s],
            values[s * z.cache_rows : (s + 1) * z.cache_rows, :],
            preferred_element_type=jnp.float32,
        )
        result = (result + rests[s][0]) / rests[s][1]
        decoded[s * z.heads : (s + 1) * z.heads, :] = jnp.where(
            table[s] >= 0, result, 0.0
        ).astype(jnp.bfloat16)


def swap(x, n, by):
    return lax.ppermute(x, "seq", [(i, i ^ by) for i in range(n)])


def on_small(
    z,
    span_queries,
    span_keys,
    span_values,
    prefix_keys,
    prefix_values,
    prefix_lengths,
    decode_queries,
    decode_new_keys,
    decode_new_values,
    decode_key_cache,
    decode_value_cache,
    owner_map,
    decode_lengths,
):
    def flat(x):
        return x.reshape(-1, z.dim)

    def local(x):
        return pltpu.with_memory_space_constraint(x, pltpu.VMEM)

    smem = pl.BlockSpec(memory_space=pltpu.SMEM)
    vmem = pl.BlockSpec(memory_space=pltpu.VMEM)
    hbm = pl.BlockSpec(memory_space=pl.ANY)

    def ints(x):
        return pltpu.with_memory_space_constraint(x, pltpu.SMEM)

    queries = flat(span_queries)
    far_queries = local(swap(queries, z.n, z.far))
    packed = pl.pallas_call(
        pack_kernel(z),
        out_shape=pltpu.VMEM((z.pack, z.dim), jnp.bfloat16),
        in_specs=[hbm] * 7,
        out_specs=vmem,
        scratch_shapes=[
            pltpu.VMEM((2, z.asks * z.kv, z.dim), jnp.bfloat16),
            pltpu.SemaphoreType.DMA((7,)),
        ],
        name="pack",
    )(
        flat(prefix_keys),
        flat(span_keys),
        flat(prefix_values),
        flat(span_values),
        flat(decode_queries),
        flat(decode_new_keys),
        flat(decode_new_values),
    )
    near = [local(packed)]
    for j in z.offsets[1:]:
        near.append(local(swap(packed, z.n, j)))
    table = pl.pallas_call(
        plan_kernel(z),
        out_shape=pltpu.SMEM((3 * z.slots + z.n,), jnp.int32),
        in_specs=[smem] * 3,
        out_specs=smem,
        name="plan",
    )(owner_map.reshape(-1), prefix_lengths, decode_lengths)
    table = ints(table)
    asked = pl.pallas_call(
        select_kernel(z),
        out_shape=pltpu.VMEM((z.picks, z.dim), jnp.bfloat16),
        in_specs=[smem] + [vmem] * z.half,
        out_specs=vmem,
        name="select",
    )(table, *near)
    wide = [pltpu.VMEM((z.rows, z.cols), jnp.float32), pltpu.VMEM((z.rows, z.cols), jnp.bfloat16)]
    wide += [pltpu.VMEM((z.rows, z.dim), jnp.float32)] * 2
    sent = pl.pallas_call(
        far_kernel(z),
        out_shape=pltpu.VMEM((z.back, z.dim), jnp.bfloat16),
        in_specs=[smem] + [vmem] * (2 + z.half),
        out_specs=vmem,
        scratch_shapes=wide,
        name="far_part",
    )(table, far_queries, local(asked), *near)
    back = local(swap(sent, z.n, z.far))
    held = pl.pallas_call(
        own_kernel(z),
        out_shape=[
            pltpu.VMEM((z.rows, z.dim), jnp.float32),
            pltpu.VMEM((8, z.rows), jnp.float32),
            pltpu.VMEM((z.picks, z.dim), jnp.bfloat16),
        ],
        in_specs=[smem] + [vmem] * (1 + z.half),
        out_specs=[vmem] * 3,
        scratch_shapes=wide,
        name="own_part",
    )(table, local(queries), *near)
    out, decoded = pl.pallas_call(
        last_kernel(z),
        out_shape=[
            jax.ShapeDtypeStruct((z.rows, z.dim), jnp.bfloat16),
            jax.ShapeDtypeStruct((z.slots * z.heads, z.dim), jnp.bfloat16),
        ],
        in_specs=[smem] + [vmem] * 6,
        out_specs=[hbm, hbm],
        scratch_shapes=[
            pltpu.VMEM((z.rows, z.dim), jnp.bfloat16),
            pltpu.VMEM((z.slots * z.heads, z.dim), jnp.bfloat16),
            pltpu.SemaphoreType.DMA((2,)),
        ],
        name="last_part",
    )(
        table,
        *[local(x) for x in held],
        back,
        local(flat(decode_key_cache)),
        local(flat(decode_value_cache)),
    )
    return (
        out.reshape(z.tokens, z.heads, z.dim),
        decoded.reshape(z.slots, z.heads, z.dim),
    )


def solution(mesh):
    group = mesh.shape["seq"]

    def on_device(*args):
        z = Sizes(group, args[0], args[1], args[3], args[6], args[9])
        if z.fits():
            return on_small(z, *args)
        return on_large(*args)

    return jax.shard_map(
        on_device,
        mesh=mesh,
        in_specs=(
            P(("groups", "seq"), "tp", None),
            P(("groups", "seq"), "tp", None),
            P(("groups", "seq"), "tp", None),
            P(("groups", "seq"), "tp", None),
            P(("groups", "seq"), "tp", None),
            P("groups"),
            P(("groups", "seq"), "tp", None),
            P(("groups", "seq"), "tp", None),
            P(("groups", "seq"), "tp", None),
            P(("groups", "seq"), None, "tp", None),
            P(("groups", "seq"), None, "tp", None),
            P("groups", None),
            P("groups"),
        ),
        out_specs=(P(("groups", "seq"), "tp", None), P(("groups", "seq"), "tp", None)),
        check_vma=False,
    )
```

```python
import math

import jax
import jax.numpy as jnp
from jax import lax
from jax.experimental import pallas as pl
from jax.experimental.pallas import tpu as pltpu
from jax.sharding import PartitionSpec as P


LOWEST = -1e30
FAR_AWAY = 1 << 30
PIECES = 8


def lookup_small(table, wanted):
    columns = jnp.arange(table.shape[0], dtype=jnp.int32)
    return jnp.sum(jnp.where(wanted[:, None] == columns[None, :], table[None, :], 0), axis=1)


def block_split(length):
    blocks = 1
    while length // blocks > 512 or length % blocks != 0:
        blocks += 1
    return blocks


def online_step(carried, queries, key_rows, value_rows, allowed):
    running_max, normalizer, weighted = carried
    scale = queries.shape[-1] ** (-0.5)
    scores = (
        jnp.einsum("tkgd,nkd->tkgn", queries, key_rows, preferred_element_type=jnp.float32) * scale
    )
    visible = allowed[:, None, None, :]
    scores = jnp.where(visible, scores, LOWEST)
    new_max = jnp.maximum(running_max, jnp.max(scores, axis=-1))
    weights = jnp.where(visible, jnp.exp(scores - new_max[..., None]), 0.0)
    factor = jnp.exp(running_max - new_max)
    normalizer = normalizer * factor + jnp.sum(weights, axis=-1)
    weighted = weighted * factor[..., None] + jnp.einsum(
        "tkgn,nkd->tkgd",
        weights.astype(jnp.bfloat16),
        value_rows,
        preferred_element_type=jnp.float32,
    )
    return (new_max, normalizer, weighted)


def guarded_step(carried, queries, key_rows, value_rows, allowed):
    return lax.cond(
        jnp.any(allowed),
        lambda inner: online_step(inner, queries, key_rows, value_rows, allowed),
        lambda inner: inner,
        carried,
    )


def fold_rows(carried, queries, key_rows, value_rows, allowed):
    length = key_rows.shape[0]
    blocks = block_split(length)
    if blocks == 1:
        return guarded_step(carried, queries, key_rows, value_rows, allowed)
    width = length // blocks
    stacked = (
        key_rows.reshape((blocks, width) + key_rows.shape[1:]),
        value_rows.reshape((blocks, width) + value_rows.shape[1:]),
        allowed.reshape(allowed.shape[0], blocks, width).transpose(1, 0, 2),
    )

    def visit(inner_carry, parts):
        return (guarded_step(inner_carry, queries, parts[0], parts[1], parts[2]), None)

    carried, _ = lax.scan(visit, carried, stacked)
    return carried


def on_large(
    span_queries,
    span_keys,
    span_values,
    prefix_keys,
    prefix_values,
    prefix_lengths,
    decode_queries,
    decode_new_keys,
    decode_new_values,
    decode_key_cache,
    decode_value_cache,
    owner_map,
    decode_lengths,
):
    device = lax.axis_index("seq")
    tokens_here, heads_here, head_dim = span_queries.shape
    kv_here = span_keys.shape[1]
    group_size = heads_here // kv_here
    queries = span_queries.reshape(tokens_here, kv_here, group_size, head_dim)
    token_index = device * tokens_here + jnp.arange(tokens_here, dtype=jnp.int32)
    prefix_here = prefix_keys.shape[0]
    initial = (
        jnp.full((tokens_here, kv_here, group_size), LOWEST, jnp.float32),
        jnp.zeros((tokens_here, kv_here, group_size), jnp.float32),
        jnp.zeros((tokens_here, kv_here, group_size, head_dim), jnp.float32),
    )
    stride = prefix_here + tokens_here
    both_keys = jnp.concatenate([prefix_keys, span_keys], axis=0)
    both_values = jnp.concatenate([prefix_values, span_values], axis=0)
    carried = initial
    key_rows = lax.all_gather(both_keys, "seq", axis=0, tiled=True)
    value_rows = lax.all_gather(both_values, "seq", axis=0, tiled=True)
    length = key_rows.shape[0]
    shards = length // stride
    tail = key_rows.shape[1:]
    keys_split = key_rows.reshape((shards, stride) + tail)
    values_split = value_rows.reshape((shards, stride) + tail)
    prefix_k = keys_split[:, :prefix_here].reshape((shards * prefix_here,) + tail)
    prefix_v = values_split[:, :prefix_here].reshape((shards * prefix_here,) + tail)
    span_k = keys_split[:, prefix_here:].reshape((shards * tokens_here,) + tail)
    span_v = values_split[:, prefix_here:].reshape((shards * tokens_here,) + tail)
    prefix_position = jnp.arange(shards * prefix_here, dtype=jnp.int32)
    prefix_ok = prefix_position % prefix_here < lookup_small(
        prefix_lengths, prefix_position // prefix_here
    )
    carried = fold_rows(
        carried,
        queries,
        prefix_k,
        prefix_v,
        jnp.broadcast_to(prefix_ok[None, :], (tokens_here, prefix_k.shape[0])),
    )
    span_position = jnp.arange(shards * tokens_here, dtype=jnp.int32)
    carried = fold_rows(
        carried, queries, span_k, span_v, span_position[None, :] <= token_index[:, None]
    )
    _, normalizer, weighted = carried
    prefill_out = (
        (weighted / normalizer[..., None])
        .reshape(tokens_here, heads_here, head_dim)
        .astype(jnp.bfloat16)
    )
    owners = owner_map[:, 0]
    requests = owners.shape[0]
    order = jnp.arange(requests, dtype=jnp.int32)
    earlier = (owners[None, :] == owners[:, None]) & (order[None, :] < order[:, None])
    ranking = jnp.sum(earlier.astype(jnp.int32), axis=1)
    slots_here = decode_key_cache.shape[0]
    slot_ids = jnp.arange(slots_here, dtype=jnp.int32)
    query_rows = lax.all_gather(decode_queries, "seq", axis=0, tiled=True)
    new_keys = lax.all_gather(decode_new_keys, "seq", axis=0, tiled=True)
    new_values = lax.all_gather(decode_new_values, "seq", axis=0, tiled=True)
    chosen = (owners == device)[None, :] & (ranking[None, :] == slot_ids[:, None])
    selector = chosen.astype(jnp.bfloat16)
    picked_queries = jnp.einsum(
        "sn,nhd->shd", selector, query_rows, preferred_element_type=jnp.float32
    )
    picked_keys = jnp.einsum("sn,nkd->skd", selector, new_keys, preferred_element_type=jnp.float32)
    picked_values = jnp.einsum(
        "sn,nkd->skd", selector, new_values, preferred_element_type=jnp.float32
    )
    picked_lengths = jnp.sum(jnp.where(chosen, decode_lengths[None, :], 0), axis=1)
    context = decode_key_cache.shape[1]
    grouped = picked_queries.astype(jnp.bfloat16).reshape(slots_here, kv_here, group_size, head_dim)
    own_keys = picked_keys.astype(jnp.bfloat16)
    own_values = picked_values.astype(jnp.bfloat16)
    scale = head_dim ** (-0.5)
    scores = (
        jnp.einsum("skgd,sckd->skgc", grouped, decode_key_cache, preferred_element_type=jnp.float32)
        * scale
    )
    visible = (jnp.arange(context, dtype=jnp.int32)[None, :] < picked_lengths[:, None])[
        :, None, None, :
    ]
    scores = jnp.where(visible, scores, LOWEST)
    own_score = (
        jnp.einsum("skgd,skd->skg", grouped, own_keys, preferred_element_type=jnp.float32) * scale
    )
    top_score = jnp.maximum(jnp.max(scores, axis=-1), own_score)
    weights = jnp.where(visible, jnp.exp(scores - top_score[..., None]), 0.0)
    own_weight = jnp.exp(own_score - top_score)
    total_weight = jnp.sum(weights, axis=-1) + own_weight
    rounded_own = lax.optimization_barrier(own_weight.astype(jnp.bfloat16)).astype(jnp.float32)
    mixed = jnp.einsum(
        "skgc,sckd->skgd",
        weights.astype(jnp.bfloat16),
        decode_value_cache,
        preferred_element_type=jnp.float32,
    )
    mixed = mixed + rounded_own[..., None] * own_values.astype(jnp.float32)[:, :, None, :]
    count_here = jnp.sum((owners == device).astype(jnp.int32))
    used = (slot_ids < count_here)[:, None, None, None]
    decode_out = (
        jnp.where(used, mixed / total_weight[..., None], 0.0)
        .reshape(slots_here, heads_here, head_dim)
        .astype(jnp.bfloat16)
    )
    return (prefill_out, decode_out)


class Sizes:
    def __init__(self, group, span_queries, span_keys, prefix_keys, decode_queries, cache):
        self.n = group
        self.half = group // 2
        self.far = self.half
        self.offsets = [j for j in range(group) if not j & self.far]
        self.tokens, self.heads, self.dim = span_queries.shape
        self.kv = span_keys.shape[1]
        self.share = self.heads // self.kv
        self.rows = self.tokens * self.heads
        self.pre = prefix_keys.shape[0]
        self.pre_rows = self.pre * self.kv
        self.block = self.pre_rows + self.tokens * self.kv
        self.cols = self.half * self.block
        self.asks = decode_queries.shape[0]
        self.ask_at = 2 * self.block
        self.new_at = self.ask_at + self.asks * self.heads
        self.new_rows = 2 * self.asks * self.kv
        self.pack = self.new_at + self.new_rows
        self.slots, self.context = cache.shape[:2]
        self.cache_rows = self.context * self.kv
        self.stat_rows = PIECES * self.rows // self.dim
        self.pick_at = self.rows + self.stat_rows
        self.pick_new_at = self.slots * self.heads
        self.picks = self.pick_new_at + self.slots // 2 * self.new_rows
        self.back = self.pick_at + self.picks
        self.factor = self.dim**-0.5 * math.log2(math.e)

    def fits(self):
        power = self.n & (self.n - 1) == 0 and self.kv & (self.kv - 1) == 0
        return (
            power
            and 4 <= self.n <= 8
            and self.dim == 128
            and self.rows % 128 == 0
            and self.share % 16 == 0
            and self.block % 16 == 0
            and self.cols % 128 == 0
            and self.cache_rows % 128 == 0
            and self.kv == 2
            and self.asks == 2
            and self.slots % 4 == 0
        )


def column_tokens(z, me, table):
    lengths = [table[3 * z.slots + (me ^ j)] for j in z.offsets]
    column = lax.broadcasted_iota(jnp.int32, (8, z.cols), 1)
    block = jnp.zeros((8, z.cols), jnp.int32)
    for j in range(1, z.half):
        block = block + (column >= z.block * j).astype(jnp.int32)
    within = column - block * z.block
    live = jnp.full((8, z.cols), lengths[0], jnp.int32)
    first = jnp.full((8, z.cols), me * z.tokens, jnp.int32)
    for j in range(1, z.half):
        live = jnp.where(block == j, lengths[j], live)
        first = jnp.where(block == j, (me ^ z.offsets[j]) * z.tokens, first)
    place = within >> (z.kv.bit_length() - 1)
    token = jnp.where(
        within < z.pre_rows,
        jnp.where(place < live, -1, FAR_AWAY),
        first + place - z.pre,
    )
    head = within & (z.kv - 1)
    return [jnp.where(head == h, token, FAR_AWAY) for h in range(z.kv)]


def partial_attention(z, me, whose, query, near, table, score_ref, weight_ref, top_ref, sum_ref):
    keys = jnp.concatenate([b[0 : z.block, :] for b in near], axis=0)
    score_ref[...] = lax.dot_general(
        query[...], keys, (((1,), (1,)), ((), ())), preferred_element_type=jnp.float32
    )
    tokens = column_tokens(z, me, table)
    for t in range(z.tokens):
        for h in range(z.kv):
            at = t * z.heads + h * z.share
            seen = tokens[h] <= whose * z.tokens + t
            scores = score_ref[at : at + z.share, :].reshape(z.share // 8, 8, z.cols)
            scores = jnp.where(seen[None], scores, LOWEST)
            top = jnp.max(scores, axis=-1, keepdims=True)
            weights = jnp.exp2((scores - top) * z.factor)
            total = jnp.sum(weights, axis=-1, keepdims=True)
            flat = (z.share, z.dim)
            wide = (z.share // 8, 8, z.dim)
            top_ref[at : at + z.share, :] = jnp.broadcast_to(top, wide).reshape(flat)
            sum_ref[at : at + z.share, :] = jnp.broadcast_to(total, wide).reshape(flat)
            weight_ref[at : at + z.share, :] = weights.reshape(z.share, z.cols).astype(jnp.bfloat16)
    values = jnp.concatenate([b[z.block : 2 * z.block, :] for b in near], axis=0)
    return jnp.dot(weight_ref[...], values, preferred_element_type=jnp.float32)


def plan_kernel(z):
    def body(owners, lengths, cached, table):
        me = lax.axis_index("seq")
        partner = me ^ z.far
        for i in range(2 * z.slots):
            table[i] = -1

        def visit(r, counts):
            mine = owners[r] == me
            theirs = owners[r] == partner

            @pl.when(mine)
            def _():
                table[counts[0]] = r
                table[2 * z.slots + counts[0]] = cached[r]

            @pl.when(theirs)
            def _():
                table[z.slots + counts[1]] = r

            return (counts[0] + mine.astype(jnp.int32), counts[1] + theirs.astype(jnp.int32))

        lax.fori_loop(0, z.n * z.asks, visit, (jnp.int32(0), jnp.int32(0)))
        for i in range(z.n):
            table[3 * z.slots + i] = lengths[i]

    return body


def pick_near(z, me, near, request):
    ask = jnp.zeros((z.heads, z.dim), jnp.bfloat16)
    new = jnp.zeros((z.new_rows, z.dim), jnp.bfloat16)
    for j in range(z.half):
        for a in range(z.asks):
            hit = request == (me ^ z.offsets[j]) * z.asks + a
            at = z.ask_at + a * z.heads
            ask = jnp.where(hit, near[j][at : at + z.heads, :], ask)
            if a == 0:
                new = jnp.where(
                    (request >= 0) & (lax.div(request, z.asks) == (me ^ z.offsets[j])),
                    near[j][z.new_at : z.pack, :],
                    new,
                )
    return ask, new


def pieces_of(x):
    first = x.astype(jnp.bfloat16).astype(jnp.float32)
    second = (x - first).astype(jnp.bfloat16).astype(jnp.float32)
    third = (x - first - second).astype(jnp.bfloat16).astype(jnp.float32)
    return [first, second, third]


def pack_kernel(z):
    def body(*refs):
        out, new, sems = refs[-3:]
        copies, at = [], 0
        for i, ref in enumerate(refs[:7]):
            rows = ref.shape[0]
            into = out.at[pl.ds(at, rows), :] if i < 5 else new.at[i - 5]
            copies.append(pltpu.make_async_copy(ref, into, sems.at[i]))
            at += rows
        for copy in reversed(copies):
            copy.start()
        for copy in reversed(copies):
            copy.wait()
        both = [new[i].astype(jnp.float32) for i in range(2)]
        out[z.new_at : z.pack, :] = jnp.concatenate(both, axis=0).astype(jnp.bfloat16)

    return body


def turn_stats(z, top_ref, sum_ref):
    lane = lax.broadcasted_iota(jnp.int32, (z.rows, z.dim), 1)
    return jnp.transpose(jnp.where(lane == 0, top_ref[...], sum_ref[...]))[:8, :]


def pick_all(z, me, table, first, near, out):
    upper = (lax.broadcasted_iota(jnp.int32, (z.new_rows, z.dim), 0) & 2) == 0
    tiles = []
    for s in range(z.slots):
        request = table[first + s]
        ask, new = pick_near(z, me, near, request)
        out[s * z.heads : (s + 1) * z.heads, :] = ask
        new = new.astype(jnp.float32)
        crossed = jnp.where(upper, pltpu.roll(new, z.new_rows - 2, 0), pltpu.roll(new, 2, 0))
        tiles.append(jnp.where((request & 1) == s % 2, new, crossed))
    for p in range(z.slots // 2):
        at = z.pick_new_at + p * z.new_rows
        tile = jnp.where(upper, tiles[2 * p], tiles[2 * p + 1])
        out[at : at + z.new_rows, :] = tile.astype(jnp.bfloat16)


def select_kernel(z):
    def body(table, *refs):
        pick_all(z, lax.axis_index("seq"), table, z.slots, refs[:-1], refs[-1])

    return body


def far_kernel(z):
    def body(table, query, asked, *refs):
        near, back, scratch = refs[: z.half], refs[z.half], refs[z.half + 1 :]
        score_ref, weight_ref, top_ref, sum_ref = scratch
        me = lax.axis_index("seq")
        back[z.pick_at : z.back, :] = asked[...]
        mixed = partial_attention(
            z, me, me ^ z.far, query, near, table, score_ref, weight_ref, top_ref, sum_ref
        )
        total = sum_ref[...]
        back[0 : z.rows, :] = (mixed / total).astype(jnp.bfloat16)
        stats = turn_stats(z, top_ref, sum_ref)
        pieces = pieces_of(stats[0:1, :]) + pieces_of(stats[1:2, :])
        row = lax.broadcasted_iota(jnp.int32, (PIECES, z.rows), 0)
        turned = jnp.zeros((PIECES, z.rows), jnp.float32)
        for i, piece in enumerate(pieces):
            turned = jnp.where(row == i, piece, turned)
        for i in range(z.rows // z.dim):
            back[z.rows + PIECES * i : z.rows + PIECES * (i + 1), :] = turned[
                :, i * z.dim : (i + 1) * z.dim
            ].astype(jnp.bfloat16)

    return body


def own_kernel(z):
    def body(table, query, *refs):
        near, (mixed, stats, mine) = refs[: z.half], refs[z.half : z.half + 3]
        score_ref, weight_ref, top_ref, sum_ref = refs[z.half + 3 :]
        me = lax.axis_index("seq")
        pick_all(z, me, table, 0, near, mine)
        mixed[...] = partial_attention(
            z, me, me, query, near, table, score_ref, weight_ref, top_ref, sum_ref
        )
        stats[...] = turn_stats(z, top_ref, sum_ref)

    return body


def last_kernel(z):
    def body(table, mixed, stats, mine, back, keys, values, *outs):
        out_hbm, decoded_hbm, out, decoded, sems = outs
        pieces = jnp.concatenate(
            [
                back[z.rows + PIECES * i : z.rows + PIECES * (i + 1), :].astype(jnp.float32)
                for i in range(z.rows // z.dim)
            ],
            axis=1,
        )
        far_top = pieces[0:1, :] + pieces[1:2, :] + pieces[2:3, :]
        far_sum = pieces[3:4, :] + pieces[4:5, :] + pieces[5:6, :]
        own_top, own_sum = stats[0:1, :], stats[1:2, :]
        top = jnp.maximum(own_top, far_top)
        here = jnp.exp2((own_top - top) * z.factor)
        there = jnp.exp2((far_top - top) * z.factor) * far_sum
        inverse = 1.0 / (own_sum * here + there)
        row = lax.broadcasted_iota(jnp.int32, (z.dim, z.rows), 0)
        shares = jnp.transpose(jnp.where(row == 0, here * inverse, there * inverse))
        joined = (
            mixed[...] * shares[:, 0:1] + back[0 : z.rows, :].astype(jnp.float32) * shares[:, 1:2]
        )
        out[...] = joined.astype(jnp.bfloat16)
        first_copy = pltpu.make_async_copy(out, out_hbm, sems.at[0])
        first_copy.start()
        decode(z, table, mine, back, keys, values, decoded)
        second_copy = pltpu.make_async_copy(decoded, decoded_hbm, sems.at[1])
        second_copy.start()
        first_copy.wait()
        second_copy.wait()

    return body


def decode(z, table, mine, back, keys, values, decoded):
    me = lax.axis_index("seq")
    column = lax.broadcasted_iota(jnp.int32, (z.heads, z.cache_rows), 1)
    row = lax.broadcasted_iota(jnp.int32, (z.heads, z.cache_rows), 0)
    shift = z.share.bit_length() - 1
    match = (column & (z.kv - 1)) == (row >> shift)
    place = column >> (z.kv.bit_length() - 1)
    head_of = lax.broadcasted_iota(jnp.int32, (z.heads, z.dim), 0) >> shift
    asks, news, scores = [], [], []
    for s in range(z.slots):
        source = lax.div(jnp.maximum(table[s], 0), z.asks)
        from_far = ((source ^ me) & z.far) != 0
        here = s * z.heads
        there = z.pick_at + here
        ask = back[there : there + z.heads, :]
        asks.append(jnp.where(from_far, ask, mine[here : here + z.heads, :]))
        here = z.pick_new_at + s // 2 * z.new_rows
        there = z.pick_at + here
        new = back[there : there + z.new_rows, :]
        new = jnp.where(from_far, new, mine[here : here + z.new_rows, :])
        news.append(new.astype(jnp.float32))
    for s in range(z.slots):
        scores.append(
            lax.dot_general(
                asks[s],
                keys[s * z.cache_rows : (s + 1) * z.cache_rows, :],
                (((1,), (1,)), ((), ())),
                preferred_element_type=jnp.float32,
            )
        )
    weights, rests = [], []
    for s in range(z.slots):
        new = news[s]
        i = s % 2 * z.kv
        new_key = jnp.where(head_of == 0, new[i : i + 1, :], new[i + 1 : i + 2, :])
        i = i + z.asks * z.kv
        new_value = jnp.where(head_of == 0, new[i : i + 1, :], new[i + 1 : i + 2, :])
        own = jnp.sum(asks[s].astype(jnp.float32) * new_key, axis=-1, keepdims=True)
        seen = jnp.where(match & (place < table[2 * z.slots + s]), scores[s], LOWEST)
        peak = jnp.maximum(jnp.max(seen, axis=-1, keepdims=True), own)
        weight = jnp.exp2((seen - peak) * z.factor)
        own_weight = jnp.exp2((own - peak) * z.factor)
        total = jnp.sum(weight, axis=-1, keepdims=True) + own_weight
        weights.append(weight.astype(jnp.bfloat16))
        rests.append((own_weight.astype(jnp.bfloat16).astype(jnp.float32) * new_value, total))
    for s in range(z.slots):
        result = jnp.dot(
            weights[s],
            values[s * z.cache_rows : (s + 1) * z.cache_rows, :],
            preferred_element_type=jnp.float32,
        )
        result = (result + rests[s][0]) / rests[s][1]
        decoded[s * z.heads : (s + 1) * z.heads, :] = jnp.where(
            table[s] >= 0, result, 0.0
        ).astype(jnp.bfloat16)


def swap(x, n, by):
    return lax.ppermute(x, "seq", [(i, i ^ by) for i in range(n)])


def on_small(
    z,
    span_queries,
    span_keys,
    span_values,
    prefix_keys,
    prefix_values,
    prefix_lengths,
    decode_queries,
    decode_new_keys,
    decode_new_values,
    decode_key_cache,
    decode_value_cache,
    owner_map,
    decode_lengths,
):
    def flat(x):
        return x.reshape(-1, z.dim)

    def local(x):
        return pltpu.with_memory_space_constraint(x, pltpu.VMEM)

    smem = pl.BlockSpec(memory_space=pltpu.SMEM)
    vmem = pl.BlockSpec(memory_space=pltpu.VMEM)
    hbm = pl.BlockSpec(memory_space=pl.ANY)

    def ints(x):
        return pltpu.with_memory_space_constraint(x, pltpu.SMEM)

    queries = flat(span_queries)
    far_queries = local(swap(queries, z.n, z.far))
    packed = pl.pallas_call(
        pack_kernel(z),
        out_shape=pltpu.VMEM((z.pack, z.dim), jnp.bfloat16),
        in_specs=[hbm] * 7,
        out_specs=vmem,
        scratch_shapes=[
            pltpu.VMEM((2, z.asks * z.kv, z.dim), jnp.bfloat16),
            pltpu.SemaphoreType.DMA((7,)),
        ],
        name="pack",
    )(
        flat(prefix_keys),
        flat(span_keys),
        flat(prefix_values),
        flat(span_values),
        flat(decode_queries),
        flat(decode_new_keys),
        flat(decode_new_values),
    )
    near = [local(packed)]
    for j in z.offsets[1:]:
        near.append(local(swap(packed, z.n, j)))
    table = pl.pallas_call(
        plan_kernel(z),
        out_shape=pltpu.SMEM((3 * z.slots + z.n,), jnp.int32),
        in_specs=[smem] * 3,
        out_specs=smem,
        name="plan",
    )(owner_map.reshape(-1), prefix_lengths, decode_lengths)
    table = ints(table)
    asked = pl.pallas_call(
        select_kernel(z),
        out_shape=pltpu.VMEM((z.picks, z.dim), jnp.bfloat16),
        in_specs=[smem] + [vmem] * z.half,
        out_specs=vmem,
        name="select",
    )(table, *near)
    wide = [pltpu.VMEM((z.rows, z.cols), jnp.float32), pltpu.VMEM((z.rows, z.cols), jnp.bfloat16)]
    wide += [pltpu.VMEM((z.rows, z.dim), jnp.float32)] * 2
    sent = pl.pallas_call(
        far_kernel(z),
        out_shape=pltpu.VMEM((z.back, z.dim), jnp.bfloat16),
        in_specs=[smem] + [vmem] * (2 + z.half),
        out_specs=vmem,
        scratch_shapes=wide,
        name="far_part",
    )(table, far_queries, local(asked), *near)
    back = local(swap(sent, z.n, z.far))
    held = pl.pallas_call(
        own_kernel(z),
        out_shape=[
            pltpu.VMEM((z.rows, z.dim), jnp.float32),
            pltpu.VMEM((8, z.rows), jnp.float32),
            pltpu.VMEM((z.picks, z.dim), jnp.bfloat16),
        ],
        in_specs=[smem] + [vmem] * (1 + z.half),
        out_specs=[vmem] * 3,
        scratch_shapes=wide,
        name="own_part",
    )(table, local(queries), *near)
    out, decoded = pl.pallas_call(
        last_kernel(z),
        out_shape=[
            jax.ShapeDtypeStruct((z.rows, z.dim), jnp.bfloat16),
            jax.ShapeDtypeStruct((z.slots * z.heads, z.dim), jnp.bfloat16),
        ],
        in_specs=[smem] + [vmem] * 6,
        out_specs=[hbm, hbm],
        scratch_shapes=[
            pltpu.VMEM((z.rows, z.dim), jnp.bfloat16),
            pltpu.VMEM((z.slots * z.heads, z.dim), jnp.bfloat16),
            pltpu.SemaphoreType.DMA((2,)),
        ],
        name="last_part",
    )(
        table,
        *[local(x) for x in held],
        back,
        local(flat(decode_key_cache)),
        local(flat(decode_value_cache)),
    )
    return (
        out.reshape(z.tokens, z.heads, z.dim),
        decoded.reshape(z.slots, z.heads, z.dim),
    )


def solution(mesh):
    group = mesh.shape["seq"]

    def on_device(*args):
        z = Sizes(group, args[0], args[1], args[3], args[6], args[9])
        if z.fits():
            return on_small(z, *args)
        return on_large(*args)

    return jax.shard_map(
        on_device,
        mesh=mesh,
        in_specs=(
            P(("groups", "seq"), "tp", None),
            P(("groups", "seq"), "tp", None),
            P(("groups", "seq"), "tp", None),
            P(("groups", "seq"), "tp", None),
            P(("groups", "seq"), "tp", None),
            P("groups"),
            P(("groups", "seq"), "tp", None),
            P(("groups", "seq"), "tp", None),
            P(("groups", "seq"), "tp", None),
            P(("groups", "seq"), None, "tp", None),
            P(("groups", "seq"), None, "tp", None),
            P("groups", None),
            P("groups"),
        ),
        out_specs=(P(("groups", "seq"), "tp", None), P(("groups", "seq"), "tp", None)),
        check_vma=False,
    )
```

```python
import math

import jax
import jax.numpy as jnp
from jax import lax
from jax.experimental import pallas as pl
from jax.experimental.pallas import tpu as pltpu
from jax.sharding import PartitionSpec as P


LOWEST = -1e30
FAR_AWAY = 1 << 30
PIECES = 8


def lookup_small(table, wanted):
    columns = jnp.arange(table.shape[0], dtype=jnp.int32)
    return jnp.sum(jnp.where(wanted[:, None] == columns[None, :], table[None, :], 0), axis=1)


def block_split(length):
    blocks = 1
    while length // blocks > 512 or length % blocks != 0:
        blocks += 1
    return blocks


def online_step(carried, queries, key_rows, value_rows, allowed):
    running_max, normalizer, weighted = carried
    scale = queries.shape[-1] ** (-0.5)
    scores = (
        jnp.einsum("tkgd,nkd->tkgn", queries, key_rows, preferred_element_type=jnp.float32) * scale
    )
    visible = allowed[:, None, None, :]
    scores = jnp.where(visible, scores, LOWEST)
    new_max = jnp.maximum(running_max, jnp.max(scores, axis=-1))
    weights = jnp.where(visible, jnp.exp(scores - new_max[..., None]), 0.0)
    factor = jnp.exp(running_max - new_max)
    normalizer = normalizer * factor + jnp.sum(weights, axis=-1)
    weighted = weighted * factor[..., None] + jnp.einsum(
        "tkgn,nkd->tkgd",
        weights.astype(jnp.bfloat16),
        value_rows,
        preferred_element_type=jnp.float32,
    )
    return (new_max, normalizer, weighted)


def guarded_step(carried, queries, key_rows, value_rows, allowed):
    return lax.cond(
        jnp.any(allowed),
        lambda inner: online_step(inner, queries, key_rows, value_rows, allowed),
        lambda inner: inner,
        carried,
    )


def fold_rows(carried, queries, key_rows, value_rows, allowed):
    length = key_rows.shape[0]
    blocks = block_split(length)
    if blocks == 1:
        return guarded_step(carried, queries, key_rows, value_rows, allowed)
    width = length // blocks
    stacked = (
        key_rows.reshape((blocks, width) + key_rows.shape[1:]),
        value_rows.reshape((blocks, width) + value_rows.shape[1:]),
        allowed.reshape(allowed.shape[0], blocks, width).transpose(1, 0, 2),
    )

    def visit(inner_carry, parts):
        return (guarded_step(inner_carry, queries, parts[0], parts[1], parts[2]), None)

    carried, _ = lax.scan(visit, carried, stacked)
    return carried


def on_large(
    span_queries,
    span_keys,
    span_values,
    prefix_keys,
    prefix_values,
    prefix_lengths,
    decode_queries,
    decode_new_keys,
    decode_new_values,
    decode_key_cache,
    decode_value_cache,
    owner_map,
    decode_lengths,
):
    device = lax.axis_index("seq")
    tokens_here, heads_here, head_dim = span_queries.shape
    kv_here = span_keys.shape[1]
    group_size = heads_here // kv_here
    queries = span_queries.reshape(tokens_here, kv_here, group_size, head_dim)
    token_index = device * tokens_here + jnp.arange(tokens_here, dtype=jnp.int32)
    prefix_here = prefix_keys.shape[0]
    initial = (
        jnp.full((tokens_here, kv_here, group_size), LOWEST, jnp.float32),
        jnp.zeros((tokens_here, kv_here, group_size), jnp.float32),
        jnp.zeros((tokens_here, kv_here, group_size, head_dim), jnp.float32),
    )
    stride = prefix_here + tokens_here
    both_keys = jnp.concatenate([prefix_keys, span_keys], axis=0)
    both_values = jnp.concatenate([prefix_values, span_values], axis=0)
    carried = initial
    key_rows = lax.all_gather(both_keys, "seq", axis=0, tiled=True)
    value_rows = lax.all_gather(both_values, "seq", axis=0, tiled=True)
    length = key_rows.shape[0]
    shards = length // stride
    tail = key_rows.shape[1:]
    keys_split = key_rows.reshape((shards, stride) + tail)
    values_split = value_rows.reshape((shards, stride) + tail)
    prefix_k = keys_split[:, :prefix_here].reshape((shards * prefix_here,) + tail)
    prefix_v = values_split[:, :prefix_here].reshape((shards * prefix_here,) + tail)
    span_k = keys_split[:, prefix_here:].reshape((shards * tokens_here,) + tail)
    span_v = values_split[:, prefix_here:].reshape((shards * tokens_here,) + tail)
    prefix_position = jnp.arange(shards * prefix_here, dtype=jnp.int32)
    prefix_ok = prefix_position % prefix_here < lookup_small(
        prefix_lengths, prefix_position // prefix_here
    )
    carried = fold_rows(
        carried,
        queries,
        prefix_k,
        prefix_v,
        jnp.broadcast_to(prefix_ok[None, :], (tokens_here, prefix_k.shape[0])),
    )
    span_position = jnp.arange(shards * tokens_here, dtype=jnp.int32)
    carried = fold_rows(
        carried, queries, span_k, span_v, span_position[None, :] <= token_index[:, None]
    )
    _, normalizer, weighted = carried
    prefill_out = (
        (weighted / normalizer[..., None])
        .reshape(tokens_here, heads_here, head_dim)
        .astype(jnp.bfloat16)
    )
    owners = owner_map[:, 0]
    requests = owners.shape[0]
    order = jnp.arange(requests, dtype=jnp.int32)
    earlier = (owners[None, :] == owners[:, None]) & (order[None, :] < order[:, None])
    ranking = jnp.sum(earlier.astype(jnp.int32), axis=1)
    slots_here = decode_key_cache.shape[0]
    slot_ids = jnp.arange(slots_here, dtype=jnp.int32)
    query_rows = lax.all_gather(decode_queries, "seq", axis=0, tiled=True)
    new_keys = lax.all_gather(decode_new_keys, "seq", axis=0, tiled=True)
    new_values = lax.all_gather(decode_new_values, "seq", axis=0, tiled=True)
    chosen = (owners == device)[None, :] & (ranking[None, :] == slot_ids[:, None])
    selector = chosen.astype(jnp.bfloat16)
    picked_queries = jnp.einsum(
        "sn,nhd->shd", selector, query_rows, preferred_element_type=jnp.float32
    )
    picked_keys = jnp.einsum("sn,nkd->skd", selector, new_keys, preferred_element_type=jnp.float32)
    picked_values = jnp.einsum(
        "sn,nkd->skd", selector, new_values, preferred_element_type=jnp.float32
    )
    picked_lengths = jnp.sum(jnp.where(chosen, decode_lengths[None, :], 0), axis=1)
    context = decode_key_cache.shape[1]
    grouped = picked_queries.astype(jnp.bfloat16).reshape(slots_here, kv_here, group_size, head_dim)
    own_keys = picked_keys.astype(jnp.bfloat16)
    own_values = picked_values.astype(jnp.bfloat16)
    scale = head_dim ** (-0.5)
    scores = (
        jnp.einsum("skgd,sckd->skgc", grouped, decode_key_cache, preferred_element_type=jnp.float32)
        * scale
    )
    visible = (jnp.arange(context, dtype=jnp.int32)[None, :] < picked_lengths[:, None])[
        :, None, None, :
    ]
    scores = jnp.where(visible, scores, LOWEST)
    own_score = (
        jnp.einsum("skgd,skd->skg", grouped, own_keys, preferred_element_type=jnp.float32) * scale
    )
    top_score = jnp.maximum(jnp.max(scores, axis=-1), own_score)
    weights = jnp.where(visible, jnp.exp(scores - top_score[..., None]), 0.0)
    own_weight = jnp.exp(own_score - top_score)
    total_weight = jnp.sum(weights, axis=-1) + own_weight
    rounded_own = lax.optimization_barrier(own_weight.astype(jnp.bfloat16)).astype(jnp.float32)
    mixed = jnp.einsum(
        "skgc,sckd->skgd",
        weights.astype(jnp.bfloat16),
        decode_value_cache,
        preferred_element_type=jnp.float32,
    )
    mixed = mixed + rounded_own[..., None] * own_values.astype(jnp.float32)[:, :, None, :]
    count_here = jnp.sum((owners == device).astype(jnp.int32))
    used = (slot_ids < count_here)[:, None, None, None]
    decode_out = (
        jnp.where(used, mixed / total_weight[..., None], 0.0)
        .reshape(slots_here, heads_here, head_dim)
        .astype(jnp.bfloat16)
    )
    return (prefill_out, decode_out)


class Sizes:
    def __init__(self, group, span_queries, span_keys, prefix_keys, decode_queries, cache):
        self.n = group
        self.half = group // 2
        self.far = self.half
        self.offsets = [j for j in range(group) if not j & self.far]
        self.tokens, self.heads, self.dim = span_queries.shape
        self.kv = span_keys.shape[1]
        self.share = self.heads // self.kv
        self.rows = self.tokens * self.heads
        self.pre = prefix_keys.shape[0]
        self.pre_rows = self.pre * self.kv
        self.block = self.pre_rows + self.tokens * self.kv
        self.cols = self.half * self.block
        self.asks = decode_queries.shape[0]
        self.ask_at = 2 * self.block
        self.new_at = self.ask_at + self.asks * self.heads
        self.new_rows = 2 * self.asks * self.kv
        self.pack = self.new_at + self.new_rows
        self.slots, self.context = cache.shape[:2]
        self.cache_rows = self.context * self.kv
        self.stat_rows = PIECES * self.rows // self.dim
        self.pick_at = self.rows + self.stat_rows
        self.pick_new_at = self.slots * self.heads
        self.picks = self.pick_new_at + self.slots // 2 * self.new_rows
        self.back = self.pick_at + self.picks
        self.factor = self.dim**-0.5 * math.log2(math.e)

    def fits(self):
        power = self.n & (self.n - 1) == 0 and self.kv & (self.kv - 1) == 0
        return (
            power
            and 4 <= self.n <= 8
            and self.dim == 128
            and self.rows % 128 == 0
            and self.share % 16 == 0
            and self.block % 16 == 0
            and self.cols % 128 == 0
            and self.cache_rows % 128 == 0
            and self.kv == 2
            and self.asks == 2
            and self.slots % 4 == 0
        )


def column_tokens(z, me, table):
    lengths = [table[3 * z.slots + (me ^ j)] for j in z.offsets]
    column = lax.broadcasted_iota(jnp.int32, (8, z.cols), 1)
    block = jnp.zeros((8, z.cols), jnp.int32)
    for j in range(1, z.half):
        block = block + (column >= z.block * j).astype(jnp.int32)
    within = column - block * z.block
    live = jnp.full((8, z.cols), lengths[0], jnp.int32)
    first = jnp.full((8, z.cols), me * z.tokens, jnp.int32)
    for j in range(1, z.half):
        live = jnp.where(block == j, lengths[j], live)
        first = jnp.where(block == j, (me ^ z.offsets[j]) * z.tokens, first)
    place = within >> (z.kv.bit_length() - 1)
    token = jnp.where(
        within < z.pre_rows,
        jnp.where(place < live, -1, FAR_AWAY),
        first + place - z.pre,
    )
    head = within & (z.kv - 1)
    return [jnp.where(head == h, token, FAR_AWAY) for h in range(z.kv)]


def partial_attention(z, me, whose, query, near, table, score_ref, weight_ref, top_ref, sum_ref):
    keys = jnp.concatenate([b[0 : z.block, :] for b in near], axis=0)
    score_ref[...] = lax.dot_general(
        query[...], keys, (((1,), (1,)), ((), ())), preferred_element_type=jnp.float32
    )
    tokens = column_tokens(z, me, table)
    for t in range(z.tokens):
        for h in range(z.kv):
            at = t * z.heads + h * z.share
            seen = tokens[h] <= whose * z.tokens + t
            scores = score_ref[at : at + z.share, :].reshape(z.share // 8, 8, z.cols)
            scores = jnp.where(seen[None], scores, LOWEST)
            top = jnp.max(scores, axis=-1, keepdims=True)
            weights = jnp.exp2((scores - top) * z.factor)
            total = jnp.sum(weights, axis=-1, keepdims=True)
            flat = (z.share, z.dim)
            wide = (z.share // 8, 8, z.dim)
            top_ref[at : at + z.share, :] = jnp.broadcast_to(top, wide).reshape(flat)
            sum_ref[at : at + z.share, :] = jnp.broadcast_to(total, wide).reshape(flat)
            weight_ref[at : at + z.share, :] = weights.reshape(z.share, z.cols).astype(jnp.bfloat16)
    values = jnp.concatenate([b[z.block : 2 * z.block, :] for b in near], axis=0)
    return jnp.dot(weight_ref[...], values, preferred_element_type=jnp.float32)


def plan_kernel(z):
    def body(owners, lengths, cached, table):
        me = lax.axis_index("seq")
        partner = me ^ z.far
        for i in range(2 * z.slots):
            table[i] = -1

        def visit(r, counts):
            mine = owners[r] == me
            theirs = owners[r] == partner

            @pl.when(mine)
            def _():
                table[counts[0]] = r
                table[2 * z.slots + counts[0]] = cached[r]

            @pl.when(theirs)
            def _():
                table[z.slots + counts[1]] = r

            return (counts[0] + mine.astype(jnp.int32), counts[1] + theirs.astype(jnp.int32))

        lax.fori_loop(0, z.n * z.asks, visit, (jnp.int32(0), jnp.int32(0)))
        for i in range(z.n):
            table[3 * z.slots + i] = lengths[i]

    return body


def pick_near(z, me, near, request):
    ask = jnp.zeros((z.heads, z.dim), jnp.bfloat16)
    new = jnp.zeros((z.new_rows, z.dim), jnp.bfloat16)
    for j in range(z.half):
        for a in range(z.asks):
            hit = request == (me ^ z.offsets[j]) * z.asks + a
            at = z.ask_at + a * z.heads
            ask = jnp.where(hit, near[j][at : at + z.heads, :], ask)
            if a == 0:
                new = jnp.where(
                    (request >= 0) & (lax.div(request, z.asks) == (me ^ z.offsets[j])),
                    near[j][z.new_at : z.pack, :],
                    new,
                )
    return ask, new


def pieces_of(x):
    first = x.astype(jnp.bfloat16).astype(jnp.float32)
    second = (x - first).astype(jnp.bfloat16).astype(jnp.float32)
    third = (x - first - second).astype(jnp.bfloat16).astype(jnp.float32)
    return [first, second, third]


def pack_kernel(z):
    def body(*refs):
        out, new, sems = refs[-3:]
        copies, at = [], 0
        for i, ref in enumerate(refs[:7]):
            rows = ref.shape[0]
            into = out.at[pl.ds(at, rows), :] if i < 5 else new.at[i - 5]
            copies.append(pltpu.make_async_copy(ref, into, sems.at[i]))
            at += rows
        for copy in copies:
            copy.start()
        for copy in copies[5:]:
            copy.wait()
        both = [new[i].astype(jnp.float32) for i in range(2)]
        out[z.new_at : z.pack, :] = jnp.concatenate(both, axis=0).astype(jnp.bfloat16)
        for copy in copies[:5]:
            copy.wait()

    return body


def turn_stats(z, top_ref, sum_ref):
    lane = lax.broadcasted_iota(jnp.int32, (z.rows, z.dim), 1)
    return jnp.transpose(jnp.where(lane == 0, top_ref[...], sum_ref[...]))[:8, :]


def pick_all(z, me, table, first, near, out):
    upper = (lax.broadcasted_iota(jnp.int32, (z.new_rows, z.dim), 0) & 2) == 0
    tiles = []
    for s in range(z.slots):
        request = table[first + s]
        ask, new = pick_near(z, me, near, request)
        out[s * z.heads : (s + 1) * z.heads, :] = ask
        new = new.astype(jnp.float32)
        crossed = jnp.where(upper, pltpu.roll(new, z.new_rows - 2, 0), pltpu.roll(new, 2, 0))
        tiles.append(jnp.where((request & 1) == s % 2, new, crossed))
    for p in range(z.slots // 2):
        at = z.pick_new_at + p * z.new_rows
        tile = jnp.where(upper, tiles[2 * p], tiles[2 * p + 1])
        out[at : at + z.new_rows, :] = tile.astype(jnp.bfloat16)


def select_kernel(z):
    def body(table, *refs):
        pick_all(z, lax.axis_index("seq"), table, z.slots, refs[:-1], refs[-1])

    return body


def far_kernel(z):
    def body(table, query, asked, *refs):
        near, back, scratch = refs[: z.half], refs[z.half], refs[z.half + 1 :]
        score_ref, weight_ref, top_ref, sum_ref = scratch
        me = lax.axis_index("seq")
        back[z.pick_at : z.back, :] = asked[...]
        mixed = partial_attention(
            z, me, me ^ z.far, query, near, table, score_ref, weight_ref, top_ref, sum_ref
        )
        total = sum_ref[...]
        back[0 : z.rows, :] = (mixed / total).astype(jnp.bfloat16)
        stats = turn_stats(z, top_ref, sum_ref)
        pieces = pieces_of(stats[0:1, :]) + pieces_of(stats[1:2, :])
        row = lax.broadcasted_iota(jnp.int32, (PIECES, z.rows), 0)
        turned = jnp.zeros((PIECES, z.rows), jnp.float32)
        for i, piece in enumerate(pieces):
            turned = jnp.where(row == i, piece, turned)
        for i in range(z.rows // z.dim):
            back[z.rows + PIECES * i : z.rows + PIECES * (i + 1), :] = turned[
                :, i * z.dim : (i + 1) * z.dim
            ].astype(jnp.bfloat16)

    return body


def own_kernel(z):
    def body(table, query, *refs):
        near, (mixed, stats, mine) = refs[: z.half], refs[z.half : z.half + 3]
        score_ref, weight_ref, top_ref, sum_ref = refs[z.half + 3 :]
        me = lax.axis_index("seq")
        pick_all(z, me, table, 0, near, mine)
        mixed[...] = partial_attention(
            z, me, me, query, near, table, score_ref, weight_ref, top_ref, sum_ref
        )
        stats[...] = turn_stats(z, top_ref, sum_ref)

    return body


def last_kernel(z):
    def body(table, mixed, stats, mine, back, keys, values, *outs):
        out_hbm, decoded_hbm, out, decoded, sems = outs
        pieces = jnp.concatenate(
            [
                back[z.rows + PIECES * i : z.rows + PIECES * (i + 1), :].astype(jnp.float32)
                for i in range(z.rows // z.dim)
            ],
            axis=1,
        )
        far_top = pieces[0:1, :] + pieces[1:2, :] + pieces[2:3, :]
        far_sum = pieces[3:4, :] + pieces[4:5, :] + pieces[5:6, :]
        own_top, own_sum = stats[0:1, :], stats[1:2, :]
        top = jnp.maximum(own_top, far_top)
        here = jnp.exp2((own_top - top) * z.factor)
        there = jnp.exp2((far_top - top) * z.factor) * far_sum
        inverse = 1.0 / (own_sum * here + there)
        row = lax.broadcasted_iota(jnp.int32, (z.dim, z.rows), 0)
        shares = jnp.transpose(jnp.where(row == 0, here * inverse, there * inverse))
        joined = (
            mixed[...] * shares[:, 0:1] + back[0 : z.rows, :].astype(jnp.float32) * shares[:, 1:2]
        )
        out[...] = joined.astype(jnp.bfloat16)
        first_copy = pltpu.make_async_copy(out, out_hbm, sems.at[0])
        first_copy.start()
        decode(z, table, mine, back, keys, values, decoded)
        second_copy = pltpu.make_async_copy(decoded, decoded_hbm, sems.at[1])
        second_copy.start()
        first_copy.wait()
        second_copy.wait()

    return body


def decode(z, table, mine, back, keys, values, decoded):
    me = lax.axis_index("seq")
    column = lax.broadcasted_iota(jnp.int32, (z.heads, z.cache_rows), 1)
    row = lax.broadcasted_iota(jnp.int32, (z.heads, z.cache_rows), 0)
    shift = z.share.bit_length() - 1
    match = (column & (z.kv - 1)) == (row >> shift)
    place = column >> (z.kv.bit_length() - 1)
    head_of = lax.broadcasted_iota(jnp.int32, (z.heads, z.dim), 0) >> shift
    asks, news, scores = [], [], []
    for s in range(z.slots):
        source = lax.div(jnp.maximum(table[s], 0), z.asks)
        from_far = ((source ^ me) & z.far) != 0
        here = s * z.heads
        there = z.pick_at + here
        ask = back[there : there + z.heads, :]
        asks.append(jnp.where(from_far, ask, mine[here : here + z.heads, :]))
        here = z.pick_new_at + s // 2 * z.new_rows
        there = z.pick_at + here
        new = back[there : there + z.new_rows, :]
        new = jnp.where(from_far, new, mine[here : here + z.new_rows, :])
        news.append(new.astype(jnp.float32))
    for s in range(z.slots):
        scores.append(
            lax.dot_general(
                asks[s],
                keys[s * z.cache_rows : (s + 1) * z.cache_rows, :],
                (((1,), (1,)), ((), ())),
                preferred_element_type=jnp.float32,
            )
        )
    weights, rests = [], []
    for s in range(z.slots):
        new = news[s]
        i = s % 2 * z.kv
        new_key = jnp.where(head_of == 0, new[i : i + 1, :], new[i + 1 : i + 2, :])
        i = i + z.asks * z.kv
        new_value = jnp.where(head_of == 0, new[i : i + 1, :], new[i + 1 : i + 2, :])
        own = jnp.sum(asks[s].astype(jnp.float32) * new_key, axis=-1, keepdims=True)
        seen = jnp.where(match & (place < table[2 * z.slots + s]), scores[s], LOWEST)
        peak = jnp.maximum(jnp.max(seen, axis=-1, keepdims=True), own)
        weight = jnp.exp2((seen - peak) * z.factor)
        own_weight = jnp.exp2((own - peak) * z.factor)
        total = jnp.sum(weight, axis=-1, keepdims=True) + own_weight
        weights.append(weight.astype(jnp.bfloat16))
        rests.append((own_weight.astype(jnp.bfloat16).astype(jnp.float32) * new_value, total))
    for s in range(z.slots):
        result = jnp.dot(
            weights[s],
            values[s * z.cache_rows : (s + 1) * z.cache_rows, :],
            preferred_element_type=jnp.float32,
        )
        result = (result + rests[s][0]) / rests[s][1]
        decoded[s * z.heads : (s + 1) * z.heads, :] = jnp.where(
            table[s] >= 0, result, 0.0
        ).astype(jnp.bfloat16)


def swap(x, n, by):
    return lax.ppermute(x, "seq", [(i, i ^ by) for i in range(n)])


def on_small(
    z,
    span_queries,
    span_keys,
    span_values,
    prefix_keys,
    prefix_values,
    prefix_lengths,
    decode_queries,
    decode_new_keys,
    decode_new_values,
    decode_key_cache,
    decode_value_cache,
    owner_map,
    decode_lengths,
):
    def flat(x):
        return x.reshape(-1, z.dim)

    def local(x):
        return pltpu.with_memory_space_constraint(x, pltpu.VMEM)

    smem = pl.BlockSpec(memory_space=pltpu.SMEM)
    vmem = pl.BlockSpec(memory_space=pltpu.VMEM)
    hbm = pl.BlockSpec(memory_space=pl.ANY)

    def ints(x):
        return pltpu.with_memory_space_constraint(x, pltpu.SMEM)

    queries = flat(span_queries)
    far_queries = local(swap(queries, z.n, z.far))
    packed = pl.pallas_call(
        pack_kernel(z),
        out_shape=pltpu.VMEM((z.pack, z.dim), jnp.bfloat16),
        in_specs=[hbm] * 7,
        out_specs=vmem,
        scratch_shapes=[
            pltpu.VMEM((2, z.asks * z.kv, z.dim), jnp.bfloat16),
            pltpu.SemaphoreType.DMA((7,)),
        ],
        name="pack",
    )(
        flat(prefix_keys),
        flat(span_keys),
        flat(prefix_values),
        flat(span_values),
        flat(decode_queries),
        flat(decode_new_keys),
        flat(decode_new_values),
    )
    near = [local(packed)]
    for j in z.offsets[1:]:
        near.append(local(swap(packed, z.n, j)))
    table = pl.pallas_call(
        plan_kernel(z),
        out_shape=pltpu.SMEM((3 * z.slots + z.n,), jnp.int32),
        in_specs=[smem] * 3,
        out_specs=smem,
        name="plan",
    )(owner_map.reshape(-1), prefix_lengths, decode_lengths)
    table = ints(table)
    asked = pl.pallas_call(
        select_kernel(z),
        out_shape=pltpu.VMEM((z.picks, z.dim), jnp.bfloat16),
        in_specs=[smem] + [vmem] * z.half,
        out_specs=vmem,
        name="select",
    )(table, *near)
    wide = [pltpu.VMEM((z.rows, z.cols), jnp.float32), pltpu.VMEM((z.rows, z.cols), jnp.bfloat16)]
    wide += [pltpu.VMEM((z.rows, z.dim), jnp.float32)] * 2
    sent = pl.pallas_call(
        far_kernel(z),
        out_shape=pltpu.VMEM((z.back, z.dim), jnp.bfloat16),
        in_specs=[smem] + [vmem] * (2 + z.half),
        out_specs=vmem,
        scratch_shapes=wide,
        name="far_part",
    )(table, far_queries, local(asked), *near)
    back = local(swap(sent, z.n, z.far))
    held = pl.pallas_call(
        own_kernel(z),
        out_shape=[
            pltpu.VMEM((z.rows, z.dim), jnp.float32),
            pltpu.VMEM((8, z.rows), jnp.float32),
            pltpu.VMEM((z.picks, z.dim), jnp.bfloat16),
        ],
        in_specs=[smem] + [vmem] * (1 + z.half),
        out_specs=[vmem] * 3,
        scratch_shapes=wide,
        name="own_part",
    )(table, local(queries), *near)
    out, decoded = pl.pallas_call(
        last_kernel(z),
        out_shape=[
            jax.ShapeDtypeStruct((z.rows, z.dim), jnp.bfloat16),
            jax.ShapeDtypeStruct((z.slots * z.heads, z.dim), jnp.bfloat16),
        ],
        in_specs=[smem] + [vmem] * 6,
        out_specs=[hbm, hbm],
        scratch_shapes=[
            pltpu.VMEM((z.rows, z.dim), jnp.bfloat16),
            pltpu.VMEM((z.slots * z.heads, z.dim), jnp.bfloat16),
            pltpu.SemaphoreType.DMA((2,)),
        ],
        name="last_part",
    )(
        table,
        *[local(x) for x in held],
        back,
        local(flat(decode_key_cache)),
        local(flat(decode_value_cache)),
    )
    return (
        out.reshape(z.tokens, z.heads, z.dim),
        decoded.reshape(z.slots, z.heads, z.dim),
    )


def solution(mesh):
    group = mesh.shape["seq"]

    def on_device(*args):
        z = Sizes(group, args[0], args[1], args[3], args[6], args[9])
        if z.fits():
            return on_small(z, *args)
        return on_large(*args)

    return jax.shard_map(
        on_device,
        mesh=mesh,
        in_specs=(
            P(("groups", "seq"), "tp", None),
            P(("groups", "seq"), "tp", None),
            P(("groups", "seq"), "tp", None),
            P(("groups", "seq"), "tp", None),
            P(("groups", "seq"), "tp", None),
            P("groups"),
            P(("groups", "seq"), "tp", None),
            P(("groups", "seq"), "tp", None),
            P(("groups", "seq"), "tp", None),
            P(("groups", "seq"), None, "tp", None),
            P(("groups", "seq"), None, "tp", None),
            P("groups", None),
            P("groups"),
        ),
        out_specs=(P(("groups", "seq"), "tp", None), P(("groups", "seq"), "tp", None)),
        check_vma=False,
    )
```
